32 devices in a mesh: section: 4 (over z), tensor: 8 (over y, x, core).
Axes of the slice: x: 2, y: 2, z: 4, core: 2. Of those that a mesh axis runs over, the one named last changes fastest.
Arguments:
- hidden_state: bfloat16 [64, 8192], P('section'), may hold values from -6 to 6
- norm_gain: float32 [8192], replicated, may hold values from 0.5 to 1.5
- wq_old: bfloat16 [8192, 8192], P('section', 'tensor'), may hold values from -0.0625 to 0.0625
- wkv_old: bfloat16 [8192, 2048], P('tensor', 'section'), may hold values from -0.0625 to 0.0625
- kv_old: bfloat16 [8, 4096, 16, 256], P('section', 'tensor'), may hold values from -241 to 241
- page_table: int32 [64, 64], replicated, may hold values from 0 to 4095, as said below
- lengths: int32 [64], replicated, may hold values from 1 to 1023
Outputs:
- context: bfloat16 [64, 8192], P('section', 'tensor')
- kv_new: bfloat16 [64, 8, 1024, 256], P('section', 'tensor')
- wq_new: bfloat16 [8192, 8192], P(None, 'tensor')
- wkv_new: bfloat16 [8192, 2048], P(None, 'tensor')
The draws below stay inside these ranges and needn't reach their ends.
Inputs may be any that keep to these rules, and one draw needn't show every extreme that they name: `page_table`: every pool page belongs to exactly one page of one request. Each block of 512 consecutive pool pages holds exactly 8 pages of every request.
All inputs are finite; a program needn't handle non-finite values.
Results may differ from the reference program's by a relative error of at most 0.0075.
The reference program's roundings to bfloat16 on the way (of `normed`, `fresh`, `cache` and `probs`) count: a program that leaves them out, or rounds other values in their place, can miss the bound.
Values may be sent and summed in bfloat16 or wider, within the bound.
A program may use at most 128 MiB of HBM per device.

```python
import jax
import jax.numpy as jnp
from jax import lax

D = 8192
HEADS = 64
KV_HEADS = 8
HEAD_DIM = 128
PAGE = 16
REQS = 64
MAXPAGES = 64
SLOTS = 1024
POOL = 4096
POOL_BLOCKS = 8
KV_COPIES = 8


def draw_page_table(key, part):
    per_block = MAXPAGES // POOL_BLOCKS
    pool_dev = POOL // POOL_BLOCKS
    slot_keys = jax.random.split(jax.random.fold_in(key, 11), REQS)
    orders = jax.vmap(lambda item: jax.random.permutation(item, MAXPAGES))(slot_keys)
    block = orders // per_block
    within = orders % per_block
    block_keys = jax.random.split(jax.random.fold_in(key, 12), POOL_BLOCKS)
    spots = jax.vmap(lambda item: jax.random.permutation(item, pool_dev))(block_keys)
    request = jnp.arange(REQS, dtype=jnp.int32)[:, None]
    local = spots[block, request * per_block + within]
    return (block * pool_dev + local).astype(jnp.int32)


def draw_kv_old(key, part):
    shape = (KV_HEADS, POOL, PAGE, 2 * HEAD_DIM)
    base = jnp.clip(jax.random.normal(jax.random.fold_in(key, 21), shape, jnp.float32), -6.0, 6.0)
    return base.astype(jnp.bfloat16)


def touch_ends(drawn, stream_key, low, top_value):
    shape = drawn.shape
    spot = [jax.random.randint(jax.random.fold_in(stream_key, axis), (), 0, shape[axis]) for axis in range(len(shape))]
    drawn = drawn.at[tuple(spot)].set(low)
    longest = shape.index(max(shape))
    spot[longest] = (spot[longest] + 1) % shape[longest]
    return drawn.at[tuple(spot)].set(top_value)


def shard_levels(own_key, dims, cuts, smallest, top_value):
    gain, own = 1.0, jax.random.fold_in(own_key, 6)
    for dim, shards_of in cuts:
        draws = jnp.exp(jax.random.uniform(jax.random.fold_in(own, dim), (shards_of,), jnp.float32, smallest / len(cuts), top_value / len(cuts)))
        gain = gain * jnp.repeat(draws, dims[dim] // shards_of).reshape([-1 if axis == dim else 1 for axis in range(len(dims))])
    return gain


def centred(own_key, extent, deviation, most, cuts=(), kind=jnp.bfloat16):
    values = jax.random.normal(own_key, extent, jnp.float32) * deviation
    if len(cuts) > 0:
        values = shard_levels(own_key, extent, cuts, -0.22, 0.18) * values
    return jnp.clip(values, min=-most, max=most).astype(kind)


def setup_inputs(seed: int = 0) -> dict:
    key_of = jax.random.split(jax.random.key(seed), 8)
    hidden_state = centred(key_of[0], (REQS, D), 1.0, 6.0, ((0, 4),))
    norm_gain = jnp.clip(1.0 + 0.1 * jax.random.normal(key_of[1], (D,), jnp.float32), 0.5, 1.5)
    wq_old = centred(key_of[2], (D, HEADS * HEAD_DIM), D ** -0.5, 0.0625, ((0, 4), (1, 8)))
    wkv_old = centred(key_of[3], (D, KV_HEADS * 2 * HEAD_DIM), D ** -0.5, 0.0625, ((0, 8), (1, 4)))
    kv_old = draw_kv_old(jax.random.fold_in(key_of[7], 71), 0)
    page_table = draw_page_table(jax.random.fold_in(key_of[7], 71), 0)
    lengths = touch_ends(jax.random.randint(key_of[6], (REQS,), 1, SLOTS), jax.random.fold_in(key_of[6], 1), 1, SLOTS - 1).astype(jnp.int32)
    return {"hidden_state": hidden_state, "norm_gain": norm_gain, "wq_old": wq_old, "wkv_old": wkv_old, "kv_old": kv_old, "page_table": page_table, "lengths": lengths}


EPSILON = 1e-05
ROPE_BASE = 500000.0

def rotate(values, position, head_dim):
    half = head_dim // 2
    frequency = ROPE_BASE ** (-(jnp.arange(half, dtype=jnp.float32) * 2.0 / head_dim))
    angles = position.astype(jnp.float32)[:, None] * frequency[None, :]
    cosine = jnp.cos(angles)[:, None, :]
    sine = jnp.sin(angles)[:, None, :]
    first = values[..., :half]
    second = values[..., half:]
    return jnp.concatenate([first * cosine - second * sine, second * cosine + first * sine], axis=-1)

def reference(hidden_state, norm_gain, wq_old, wkv_old, kv_old, page_table, lengths):
    width = 2 * HEAD_DIM
    group = HEADS // KV_HEADS
    repeats = KV_COPIES // KV_HEADS
    widened = hidden_state.astype(jnp.float32)
    scale = lax.rsqrt(lax.optimization_barrier(jnp.mean(widened * widened, axis=1, keepdims=True)) + EPSILON)
    normed = (widened * scale * norm_gain.astype(jnp.float32)).astype(jnp.bfloat16)
    query = jnp.dot(normed, wq_old, preferred_element_type=jnp.float32).reshape(REQS, HEADS, HEAD_DIM)
    query = rotate(query, lengths, HEAD_DIM).astype(jnp.bfloat16)
    fresh = jnp.dot(normed, wkv_old, preferred_element_type=jnp.float32).reshape(REQS, KV_HEADS, width)
    fresh_key = rotate(fresh[:, :, :HEAD_DIM], lengths, HEAD_DIM)
    fresh = jnp.concatenate([fresh_key, fresh[:, :, HEAD_DIM:]], axis=2).astype(jnp.bfloat16)
    slot_ids = jnp.arange(SLOTS, dtype=jnp.int32)
    written = slot_ids[None, :] == lengths[:, None]
    visible = slot_ids[None, :] <= lengths[:, None]

    def per_head(head):
        pages = kv_old[head][page_table]
        cache = pages.reshape(REQS, SLOTS, width)
        token = lax.dynamic_index_in_dim(fresh, head, 1, keepdims=False)
        cache = jnp.where(written[:, :, None], token[:, None, :], cache)
        queries = lax.dynamic_slice_in_dim(query, head * group, group, 1).astype(jnp.float32)
        scores = jnp.einsum('rgd,rsd->rgs', queries, cache[:, :, :HEAD_DIM].astype(jnp.float32)) * HEAD_DIM ** (-0.5)
        seen = visible[:, None, :]
        peak = lax.optimization_barrier(jnp.max(jnp.where(seen, scores, -jnp.inf), axis=2, keepdims=True))
        weights = jnp.where(seen, jnp.exp(scores - peak), 0.0)
        probs = (weights / lax.optimization_barrier(jnp.sum(weights, axis=2, keepdims=True))).astype(jnp.bfloat16)
        mixed = jnp.einsum('rgs,rsd->rgd', probs.astype(jnp.float32), cache[:, :, HEAD_DIM:].astype(jnp.float32))
        return (cache, mixed.astype(jnp.bfloat16))
    caches, mixed = lax.map(per_head, jnp.arange(KV_HEADS, dtype=jnp.int32))
    context = jnp.moveaxis(mixed, 0, 1).reshape(REQS, HEADS * HEAD_DIM)
    kv_new = jnp.repeat(jnp.moveaxis(caches, 0, 1), repeats, axis=1)
    wkv_new = jnp.repeat(wkv_old.reshape(D, KV_HEADS, width), repeats, axis=1).reshape(D, KV_COPIES * width)
    return (context, kv_new, wq_old, wkv_new)
```

```python
import functools

import jax
import jax.numpy as jnp
from jax import lax
from jax.experimental import pallas as pl
from jax.experimental.pallas import tpu as pltpu
from jax.sharding import PartitionSpec as P


KV_HEADS = 8
HEAD_DIM = 128


EPSILON = 1e-05
ROPE_BASE = 500000.0
MESH = pl.DeviceIdType.MESH
CHUNKS = 8
TILES = 8
EARLY = 2
LATE = 4


def rotate(values, position, head_dim):
    half = head_dim // 2
    frequency = ROPE_BASE ** (-(jnp.arange(half, dtype=jnp.float32) * 2.0 / head_dim))
    angles = position.astype(jnp.float32)[:, None] * frequency[None, :]
    cosine = jnp.cos(angles)[:, None, :]
    sine = jnp.sin(angles)[:, None, :]
    first = values[..., :half]
    second = values[..., half:]
    return jnp.concatenate(
        [first * cosine - second * sine, second * cosine + first * sine], axis=-1
    )


def pick_kernel(count, spots_ref, kv_ref, out_ref):
    base = pl.program_id(1) * count

    def step(i, carry):
        out_ref[0, 0, i] = kv_ref[0, spots_ref[base + i]]
        return carry

    lax.fori_loop(0, count, step, 0, unroll=8)


def pick_pages(kv_old, spots, sections):
    heads, pool, page, width = kv_old.shape
    count = spots.shape[0] // sections
    return pl.pallas_call(
        functools.partial(pick_kernel, count),
        out_shape=jax.ShapeDtypeStruct((sections, heads, count, page, width), kv_old.dtype),
        grid_spec=pltpu.PrefetchScalarGridSpec(
            num_scalar_prefetch=1,
            grid=(heads, sections),
            in_specs=[pl.BlockSpec((1, pool, page, width), lambda h, s, spots: (h, 0, 0, 0))],
            out_specs=pl.BlockSpec(
                (1, 1, count, page, width), lambda h, s, spots: (s, h, 0, 0, 0)
            ),
        ),
        compiler_params=pltpu.CompilerParams(vmem_limit_bytes=40 * 2**20),
        name="pick_pages",
    )(spots, kv_old)


def exchange_kernel(
    sections,
    tensors,
    local_heads,
    repeats,
    kept,
    normed_ref,
    wq_ref,
    pages_ref,
    wkv_ref,
    part_ref,
    arrived_ref,
    wkv_new_ref,
    wq_new_ref,
    stage_ref,
    stage_wkv_ref,
    late_ref,
    held,
    spread,
    made,
    part_in,
    page_send,
    page_recv,
    wkv_send,
    wkv_recv,
    local_sem,
    own_send,
    relay_send,
    wq_recv,
    stage_send,
    stage_recv,
    wkv_own_send,
    wkv_relay_send,
    wkv_stage_recv,
    help_send,
    help_recv,
):
    me = lax.axis_index("section")
    mine = lax.axis_index("tensor")
    depth, columns = wq_ref.shape
    width = wkv_new_ref.shape[1]
    block = wkv_ref.shape[0]
    late_rows = late_ref.shape[0]
    chunks = own_send.shape[1]
    chunk = depth // chunks
    last = sections - 1
    onward = (me < last, me > 0)
    next_to = (me + 1, me - 1)
    feeds = (me == last - 1, me == 1)
    fed = (me == last, me == 0)

    def wq_rows(owner, i):
        return wq_new_ref.at[pl.ds(pl.multiple_of(owner * depth + i * chunk, 16), chunk), :]

    def own_copy(side, i):
        return pltpu.make_async_remote_copy(
            wq_ref.at[pl.ds(pl.multiple_of(i * chunk, 16), chunk), :],
            wq_rows(me, i),
            own_send.at[side, i],
            wq_recv.at[me, i],
            device_id=(next_to[side], mine),
            device_id_type=MESH,
        )

    def relay_copy(owner, side, i):
        return pltpu.make_async_remote_copy(
            wq_rows(owner, i),
            wq_rows(owner, i),
            relay_send.at[owner, i],
            wq_recv.at[owner, i],
            device_id=(next_to[side], mine),
            device_id_type=MESH,
        )

    def each_chunk(act, first=0, end=chunks):
        def run(i, carry):
            act(i)
            return carry

        lax.fori_loop(first, end, run, 0)

    def goes(side, i):
        return jnp.logical_and(
            onward[side], jnp.logical_or(jnp.logical_not(feeds[side]), i < kept)
        )

    def send_own(i):
        for side in range(2):
            pl.when(goes(side, i))(lambda: own_copy(side, i).start())

    def owner_of(side, step):
        return (me - step, me + step)[side]

    def real(side, step):
        return (me - step >= 0, me + step < sections)[side]

    def stage_copy(origin, other, step):
        return pltpu.make_async_remote_copy(
            pages_ref.at[other],
            stage_ref.at[origin],
            stage_send.at[step],
            stage_recv.at[origin],
            device_id=(other, mine),
            device_id_type=MESH,
        )

    def wkv_own_copy(side):
        return pltpu.make_async_remote_copy(
            wkv_ref,
            stage_wkv_ref.at[me],
            wkv_own_send.at[side],
            wkv_stage_recv.at[me],
            device_id=(next_to[side], mine),
            device_id_type=MESH,
        )

    def wkv_relay_copy(owner, side):
        return pltpu.make_async_remote_copy(
            stage_wkv_ref.at[owner],
            stage_wkv_ref.at[owner],
            wkv_relay_send.at[owner],
            wkv_stage_recv.at[owner],
            device_id=(next_to[side], mine),
            device_id_type=MESH,
        )

    def page_copy(step, head, copy):
        slot = (step * local_heads + head) * repeats + copy
        other = lax.rem(me + step, sections)
        target = (other * local_heads + head) * repeats + copy
        source = pages_ref.at[me, head] if step == 0 else stage_ref.at[other, head]
        here = (source, arrived_ref.at[mine])
        remote = pltpu.make_async_remote_copy(
            *here,
            page_send.at[slot],
            page_recv.at[mine],
            device_id=(me, target),
            device_id_type=MESH,
        )
        return target, remote, pltpu.make_async_copy(*here, local_sem.at[0])

    def wkv_copy(step, head, copy):
        slot = (step * local_heads + head) * repeats + copy
        other = lax.rem(me + step, sections)
        target = (other * local_heads + head) * repeats + copy
        here = (
            (wkv_ref if step == 0 else stage_wkv_ref.at[other]).at[:, pl.ds(head * width, width)],
            wkv_new_ref.at[pl.ds(pl.multiple_of(mine * block, 128), block), :],
        )
        remote = pltpu.make_async_remote_copy(
            *here,
            wkv_send.at[slot],
            wkv_recv.at[mine],
            device_id=(me, target),
            device_id_type=MESH,
        )
        return target, remote, pltpu.make_async_copy(*here, local_sem.at[1])

    def begin(make, step):
        for head in range(local_heads):
            for copy in range(repeats):
                target, remote, local = make(step, head, copy)
                pl.when(target != mine)(remote.start)
                pl.when(target == mine)(local.start)

    def spread_copy(side):
        feeder = (last - 1, 1)[side]
        start = pl.multiple_of(feeder * depth + depth - late_rows, 128)
        return pltpu.make_async_remote_copy(
            normed_ref.at[:, pl.ds(start, late_rows)],
            spread.at[side],
            help_send.at[0],
            help_recv.at[side],
            device_id=(feeder, mine),
            device_id_type=MESH,
        )

    def part_copy(side):
        return pltpu.make_async_remote_copy(
            made.at[side],
            part_in,
            help_send.at[1 + side],
            help_recv.at[2],
            device_id=((last, 0)[side], mine),
            device_id_type=MESH,
        )

    for side in range(2):
        pl.when(onward[side])(lambda: wkv_own_copy(side).start())
        pl.when(fed[side])(lambda: spread_copy(side).start())
    begin(wkv_copy, 0)
    begin(page_copy, 0)
    each_chunk(send_own)
    for step in range(sections - 1, 0, -1):
        for side in range(2):
            pl.when(real(side, step))(
                lambda: stage_copy(
                    me, owner_of(side, step), step if side else sections - step
                ).start()
            )

    take = pltpu.make_async_copy(
        wq_ref.at[pl.ds(depth - late_rows, late_rows), :], held, local_sem.at[2]
    )
    take.start()
    take.wait()
    put = pltpu.make_async_copy(held, late_ref, local_sem.at[3])
    put.start()
    tile = 256
    for side in range(2):

        @pl.when(feeds[side])
        def _():
            spread_copy(side).wait_recv()

            def product(i, carry):
                span = pl.ds(pl.multiple_of(i * tile, tile), tile)
                made[side, :, span] = jnp.dot(
                    spread[side], held[:, span], preferred_element_type=jnp.float32
                )
                return carry

            lax.fori_loop(0, columns // tile, product, 0)
            part_copy(side).start()

    def pass_wkv(step):
        for side in range(2):
            owner = owner_of(side, step)

            @pl.when(real(side, step))
            def _():
                wkv_relay_copy(owner, side).wait_recv()
                pl.when(onward[side])(lambda: wkv_relay_copy(owner, side).start())
                begin(wkv_copy, step if side else sections - step)

    def pass_wq(step):
        def pass_on(i):
            for side in range(2):
                owner = owner_of(side, step)
                there = real(side, step)
                if step == 1:
                    there = jnp.logical_and(
                        there, jnp.logical_or(jnp.logical_not(fed[side]), i < kept)
                    )

                @pl.when(there)
                def _():
                    relay_copy(owner, side, i).wait_recv()
                    pl.when(onward[side])(lambda: relay_copy(owner, side, i).start())

        each_chunk(pass_on)

    for step in range(1, sections):
        pass_wkv(step)
        pass_wq(step)
        if step == 1:
            for away in range(1, sections):
                other = lax.rem(me + away, sections)
                stage_copy(other, other, away).wait_recv()
                begin(page_copy, away)

    put.wait()
    for side in range(2):

        @pl.when(fed[side])
        def _():
            spread_copy(side).wait_send()
            part_copy(side).wait_recv()

        pl.when(feeds[side])(lambda: part_copy(side).wait_send())
    end = jnp.logical_or(fed[0], fed[1])

    @pl.when(end)
    def _():
        part_ref[...] = part_in[...]

    @pl.when(jnp.logical_not(end))
    def _():
        part_ref[...] = jnp.zeros_like(part_ref)

    def sent(i):
        for side in range(2):
            pl.when(goes(side, i))(lambda: own_copy(side, i).wait_send())
            for step in range(1, sections):
                pl.when(jnp.logical_and(real(side, step), onward[side]))(
                    lambda: relay_copy(owner_of(side, step), side, i).wait_send()
                )

    each_chunk(sent)
    for side in range(2):
        pl.when(onward[side])(lambda: wkv_own_copy(side).wait_send())
        for step in range(1, sections):
            pl.when(jnp.logical_and(real(side, step), onward[side]))(
                lambda: wkv_relay_copy(owner_of(side, step), side).wait_send()
            )
    for step in range(1, sections):
        stage_copy(me, lax.rem(me + step, sections), step).wait_send()
    for make in (page_copy, wkv_copy):
        for step in range(sections):
            for head in range(local_heads):
                for copy in range(repeats):
                    target, remote, local = make(step, head, copy)
                    pl.when(target != mine)(remote.wait_send)
                    pl.when(target == mine)(local.wait)
    for origin in range(tensors):
        pages_in = pltpu.make_async_remote_copy(
            pages_ref.at[0, 0],
            arrived_ref.at[origin],
            page_send.at[0],
            page_recv.at[origin],
            device_id=(me, origin),
            device_id_type=MESH,
        )
        wkv_in = pltpu.make_async_remote_copy(
            wkv_ref.at[:, pl.ds(0, width)],
            wkv_new_ref.at[pl.ds(origin * block, block), :],
            wkv_send.at[0],
            wkv_recv.at[origin],
            device_id=(me, origin),
            device_id_type=MESH,
        )
        outside = mine != origin
        pl.when(outside)(pages_in.wait_recv)
        pl.when(outside)(wkv_in.wait_recv)


def exchange(normed, wq_old, pages, wkv_old, sections, tensors, repeats):
    rows = normed.shape[0]
    depth, columns = wq_old.shape
    local_heads = pages.shape[1]
    width = pages.shape[4]
    copies = sections * local_heads * repeats
    late_rows = depth // TILES * LATE
    kept = CHUNKS // TILES * (TILES - EARLY - LATE)
    dma = pltpu.SemaphoreType.DMA
    vmem = pl.BlockSpec(memory_space=pltpu.VMEM)
    hbm = pl.BlockSpec(memory_space=pl.ANY)
    return pl.pallas_call(
        functools.partial(
            exchange_kernel, sections, tensors, local_heads, repeats, kept
        ),
        out_shape=(
            jax.ShapeDtypeStruct((rows, columns), jnp.float32),
            jax.ShapeDtypeStruct((tensors,) + pages.shape[2:], pages.dtype),
            jax.ShapeDtypeStruct((wkv_old.shape[0] * tensors, width), wkv_old.dtype),
            jax.ShapeDtypeStruct((depth * sections, columns), wq_old.dtype),
            jax.ShapeDtypeStruct(pages.shape, pages.dtype),
            jax.ShapeDtypeStruct((sections,) + wkv_old.shape, wkv_old.dtype),
            jax.ShapeDtypeStruct((late_rows, columns), wq_old.dtype),
        ),
        in_specs=[vmem, hbm, hbm, hbm],
        out_specs=(vmem, hbm, hbm, hbm, hbm, hbm, hbm),
        scratch_shapes=[
            pltpu.VMEM((late_rows, columns), wq_old.dtype),
            pltpu.VMEM((2, rows, late_rows), normed.dtype),
            pltpu.VMEM((2, rows, columns), jnp.float32),
            pltpu.VMEM((rows, columns), jnp.float32),
            dma((copies,)),
            dma((tensors,)),
            dma((copies,)),
            dma((tensors,)),
            dma((4,)),
            dma((2, CHUNKS)),
            dma((sections, CHUNKS)),
            dma((sections, CHUNKS)),
            dma((sections,)),
            dma((sections,)),
            dma((2,)),
            dma((sections,)),
            dma((sections,)),
            dma((3,)),
            dma((3,)),
        ],
        compiler_params=pltpu.CompilerParams(
            has_side_effects=True, vmem_limit_bytes=40 * 2**20
        ),
        cost_estimate=pl.CostEstimate(
            flops=4 * rows * late_rows * columns,
            bytes_accessed=400 * 2**20,
            transcendentals=0,
        ),
        name="exchange",
    )(normed, wq_old, pages, wkv_old)


def gather_kernel(
    sections,
    me_ref,
    normed_ref,
    part_ref,
    own_ref,
    far_ref,
    early_ref,
    wkv_ref,
    out_ref,
    query_ref,
    wkv_out_ref,
    fresh_ref,
    total,
    fresh,
):
    i = pl.program_id(0)
    me = me_ref[0]
    owner = i // TILES
    k = i % TILES
    tile = out_ref.shape[0]
    mine = owner == me
    fed = jnp.logical_or(
        jnp.logical_and(me == sections - 1, owner == sections - 2),
        jnp.logical_and(me == 0, owner == 1),
    )
    early = jnp.logical_and(
        fed, jnp.logical_and(k >= TILES - EARLY - LATE, k < TILES - LATE)
    )
    late = jnp.logical_and(fed, k >= TILES - LATE)

    @pl.when(i == 0)
    def _():
        total[...] = part_ref[...]
        fresh[...] = jnp.zeros_like(fresh)

    features = normed_ref[:, pl.ds(pl.multiple_of(i * tile, 128), tile)]
    wkv_out_ref[...] = wkv_ref[...]
    fresh[...] += jnp.dot(features, wkv_ref[...], preferred_element_type=jnp.float32)

    def keep(ref):
        out_ref[...] = ref[...]
        total[...] += jnp.dot(features, ref[...], preferred_element_type=jnp.float32)

    pl.when(mine)(lambda: keep(own_ref))
    pl.when(early)(lambda: keep(early_ref))
    other = jnp.logical_or(mine, jnp.logical_or(early, late))
    pl.when(jnp.logical_not(other))(lambda: keep(far_ref))

    @pl.when(i == pl.num_programs(0) - 1)
    def _():
        query_ref[...] = total[...]
        fresh_ref[...] = fresh[...]


def gather(me, normed, part, wq_old, far, early, wkv, sections):
    rows, total_depth = normed.shape
    depth, columns = wq_old.shape
    tile = depth // TILES
    width = wkv.shape[1]

    def own_at(i, me):
        return (jnp.clip(i - me[0] * TILES, 0, TILES - 1), 0)

    def far_at(i, me):
        own = i // TILES == me[0]
        return (jnp.where(own, jnp.maximum(me[0] * TILES - 1, 0), i), 0)

    def early_at(i, me):
        feeder = jnp.where(me[0] == sections - 1, sections - 2, 1)
        return (jnp.clip(i - feeder * TILES - (TILES - EARLY - LATE), 0, EARLY - 1), 0)

    return pl.pallas_call(
        functools.partial(gather_kernel, sections),
        out_shape=(
            jax.ShapeDtypeStruct((total_depth, columns), wq_old.dtype),
            jax.ShapeDtypeStruct((rows, columns), jnp.float32),
            jax.ShapeDtypeStruct(wkv.shape, wkv.dtype),
            jax.ShapeDtypeStruct((rows, width), jnp.float32),
        ),
        grid_spec=pltpu.PrefetchScalarGridSpec(
            num_scalar_prefetch=1,
            grid=(sections * TILES,),
            in_specs=[
                pl.BlockSpec((rows, total_depth), lambda i, me: (0, 0)),
                pl.BlockSpec((rows, columns), lambda i, me: (0, 0)),
                pl.BlockSpec((tile, columns), own_at),
                pl.BlockSpec((tile, columns), far_at),
                pl.BlockSpec((tile, columns), early_at),
                pl.BlockSpec((tile, width), lambda i, me: (i, 0)),
            ],
            out_specs=(
                pl.BlockSpec((tile, columns), lambda i, me: (i, 0)),
                pl.BlockSpec((rows, columns), lambda i, me: (0, 0)),
                pl.BlockSpec((tile, width), lambda i, me: (i, 0)),
                pl.BlockSpec((rows, width), lambda i, me: (0, 0)),
            ),
            scratch_shapes=[
                pltpu.VMEM((rows, columns), jnp.float32),
                pltpu.VMEM((rows, width), jnp.float32),
            ],
        ),
        cost_estimate=pl.CostEstimate(
            flops=2 * rows * total_depth * columns,
            bytes_accessed=4 * total_depth * columns,
            transcendentals=0,
        ),
        compiler_params=pltpu.CompilerParams(vmem_limit_bytes=40 * 2**20),
        name="gather_query",
    )(me, normed, part, wq_old, far, early, wkv)


def place_kernel(sections, depth, late_ref, held_ref, out_ref, buffer, into, out):
    me = lax.axis_index("section")
    pieces = into.shape[0]
    piece = late_ref.shape[0] // pieces
    feeder = jnp.where(me == 0, 1, sections - 2)
    start = feeder * depth + depth - late_ref.shape[0]

    def read(p):
        span = pl.ds(p * piece, piece)
        return pltpu.make_async_copy(late_ref.at[span, :], buffer.at[span, :], into.at[p])

    def write(p):
        return pltpu.make_async_copy(
            buffer.at[pl.ds(p * piece, piece), :],
            out_ref.at[pl.ds(pl.multiple_of(start + p * piece, 16), piece), :],
            out.at[p],
        )

    @pl.when(jnp.logical_or(me == 0, me == sections - 1))
    def _():
        for p in range(pieces):
            read(p).start()
        for p in range(pieces):
            read(p).wait()
            write(p).start()
        for p in range(pieces):
            write(p).wait()


def place_late(late, wq_new, sections):
    depth = wq_new.shape[0] // sections
    pieces = 4
    hbm = pl.BlockSpec(memory_space=pl.ANY)
    dma = pltpu.SemaphoreType.DMA
    return pl.pallas_call(
        functools.partial(place_kernel, sections, depth),
        out_shape=jax.ShapeDtypeStruct(wq_new.shape, wq_new.dtype),
        in_specs=[hbm, hbm],
        out_specs=hbm,
        scratch_shapes=[pltpu.VMEM(late.shape, late.dtype), dma((pieces,)), dma((pieces,))],
        input_output_aliases={1: 0},
        cost_estimate=pl.CostEstimate(
            flops=1024, bytes_accessed=4 * late.size, transcendentals=0
        ),
        name="place_late",
    )(late, wq_new)


def attend_kernel(
    pages_of, per_block, page, head_dim, place_ref, length_ref, in_ref, fresh_ref, query_ref, cache_ref, context_ref
):
    request = pl.program_id(0)
    length = length_ref[request]
    base = request * pages_of

    def order(j, carry):
        spot = place_ref[base + j]
        start = pl.multiple_of(j * page, page)
        cache_ref[0, pl.ds(start, page), :] = in_ref[
            lax.div(spot, per_block), 0, lax.rem(spot, per_block)
        ]
        return carry

    lax.fori_loop(0, pages_of, order, 0, unroll=8)
    start = pl.multiple_of(lax.div(length, page) * page, page)
    held = cache_ref[0, pl.ds(start, page), :]
    row = lax.broadcasted_iota(jnp.int32, held.shape, 0)
    fresh = jnp.broadcast_to(fresh_ref[0].astype(jnp.float32), held.shape)
    cache_ref[0, pl.ds(start, page), :] = jnp.where(
        row == lax.rem(length, page), fresh, held.astype(jnp.float32)
    ).astype(held.dtype)
    keys = cache_ref[0, :, :head_dim]
    values = cache_ref[0, :, head_dim:]
    scores = lax.dot_general(
        query_ref[0], keys, (((1,), (1,)), ((), ())), preferred_element_type=jnp.float32
    ) * head_dim ** (-0.5)
    seen = lax.broadcasted_iota(jnp.int32, scores.shape, 1) <= length
    peak = jnp.max(jnp.where(seen, scores, -jnp.inf), axis=1, keepdims=True)
    weights = jnp.where(seen, jnp.exp(scores - peak), 0.0)
    probs = (weights / jnp.sum(weights, axis=1, keepdims=True)).astype(jnp.bfloat16)
    context_ref[0] = jnp.dot(probs, values, preferred_element_type=jnp.float32).astype(
        context_ref.dtype
    )


def attend(arrived, place, lengths, fresh, query, head_dim):
    blocks, rows, per_block, page, width = arrived.shape
    pages_of = blocks * per_block
    heads = query.shape[1]
    return pl.pallas_call(
        functools.partial(attend_kernel, pages_of, per_block, page, head_dim),
        out_shape=(
            jax.ShapeDtypeStruct((rows, pages_of * page, width), arrived.dtype),
            jax.ShapeDtypeStruct(query.shape, jnp.bfloat16),
        ),
        grid_spec=pltpu.PrefetchScalarGridSpec(
            num_scalar_prefetch=2,
            grid=(rows,),
            in_specs=[
                pl.BlockSpec((blocks, 1, per_block, page, width), lambda r, *_: (0, r, 0, 0, 0)),
                pl.BlockSpec((1, 1, width), lambda r, *_: (r, 0, 0)),
                pl.BlockSpec((1, heads, head_dim), lambda r, *_: (r, 0, 0)),
            ],
            out_specs=(
                pl.BlockSpec((1, pages_of * page, width), lambda r, *_: (r, 0, 0)),
                pl.BlockSpec((1, heads, head_dim), lambda r, *_: (r, 0, 0)),
            ),
        ),
        cost_estimate=pl.CostEstimate(
            flops=4 * rows * heads * pages_of * page * head_dim,
            bytes_accessed=4 * arrived.size,
            transcendentals=rows * heads * pages_of * page,
        ),
        compiler_params=pltpu.CompilerParams(vmem_limit_bytes=40 * 2**20),
        name="attend",
    )(place.reshape(-1), lengths, arrived, fresh[:, None, :], query)


def work(hidden_state, norm_gain, wq_old, wkv_old, kv_old, page_table, lengths):
    sections = lax.axis_size("section")
    tensors = lax.axis_size("tensor")
    section_id = lax.axis_index("section")
    tensor_id = lax.axis_index("tensor")
    rows = hidden_state.shape[0]
    head_dim = HEAD_DIM
    width = 2 * head_dim
    repeats = tensors // KV_HEADS
    queries_here = wq_old.shape[1] // head_dim
    pool_dev = kv_old.shape[1]
    page = kv_old.shape[2]
    per_block = page_table.shape[1] // tensors
    widened = hidden_state.astype(jnp.float32)
    scale = lax.rsqrt(jnp.mean(widened * widened, axis=1, keepdims=True) + EPSILON)
    normed = (widened * scale * norm_gain[None, :]).astype(jnp.bfloat16)
    owner = page_table // pool_dev
    blocks = jnp.arange(tensors, dtype=jnp.int32)
    onehot = (owner[:, :, None] == blocks[None, None, :]).astype(jnp.int32)
    ranks = jnp.sum((jnp.cumsum(onehot, axis=1) - 1) * onehot, axis=2)
    mine = owner == tensor_id
    wanted = ranks[:, :, None] == jnp.arange(per_block, dtype=jnp.int32)[None, None, :]
    picks = (mine[:, :, None] & wanted).astype(jnp.int32)
    spots = jnp.sum(picks * (page_table % pool_dev)[:, :, None], axis=1)
    pages = pick_pages(kv_old, spots.reshape(-1), sections)
    depth = wq_old.shape[0]
    ends = sorted({(sections - 2, sections - 1), (1, 0)})
    early_rows = depth // TILES * EARLY
    late_rows = depth // TILES * LATE
    stop = depth - late_rows
    early = lax.ppermute(wq_old[stop - early_rows : stop], "section", ends)
    part, arrived, wkv_far, far, _, _, late = exchange(
        normed, wq_old, pages, wkv_old, sections, tensors, repeats
    )
    late = lax.ppermute(late, "section", ends)
    me = jnp.full((1,), section_id, jnp.int32)
    wq_new, query, wkv_new, fresh = gather(
        me, normed, part, wq_old, far, early, wkv_far, sections
    )
    arrived = arrived.reshape(tensors, rows, per_block, page, width)
    place = lax.dynamic_slice_in_dim(owner * per_block + ranks, section_id * rows, rows, 0)
    my_lengths = lax.dynamic_slice_in_dim(lengths, section_id * rows, rows, 0)
    fresh_key = rotate(fresh[:, None, :head_dim], my_lengths, head_dim)[:, 0]
    fresh = jnp.concatenate([fresh_key, fresh[:, head_dim:]], axis=1).astype(jnp.bfloat16)
    query = rotate(query.reshape(rows, queries_here, head_dim), my_lengths, head_dim).astype(
        jnp.bfloat16
    )
    cache, context = attend(arrived, place, my_lengths, fresh, query, head_dim)
    wq_new = place_late(late, wq_new, sections)
    return (context.reshape(rows, queries_here * head_dim), cache[:, None], wq_new, wkv_new)


def solution(mesh):
    placed = (
        P("section", None),
        P(),
        P("section", "tensor"),
        P("tensor", "section"),
        P("section", "tensor", None, None),
        P(),
        P(),
    )
    return jax.shard_map(
        work,
        mesh=mesh,
        in_specs=placed,
        out_specs=(
            P("section", "tensor"),
            P("section", "tensor", None, None),
            P(None, "tensor"),
            P(None, "tensor"),
        ),
        check_vma=False,
    )
```

```python
import functools

import jax
import jax.numpy as jnp
from jax import lax
from jax.experimental import pallas as pl
from jax.experimental.pallas import tpu as pltpu
from jax.sharding import PartitionSpec as P


KV_HEADS = 8
HEAD_DIM = 128


EPSILON = 1e-05
ROPE_BASE = 500000.0
MESH = pl.DeviceIdType.MESH
CHUNKS = 16
PIECES = 4
UNIT = 128
EARLY = 4
LATE = 6
PAIR = 8
TOGETHER = 4
VMEM_LIMIT = 60 * 2**20


def split(depth):
    tiles = depth // UNIT
    return tiles, max(1, tiles * EARLY // 16), max(1, tiles * LATE // 16)


def rotate(values, position, head_dim):
    half = head_dim // 2
    frequency = ROPE_BASE ** (-(jnp.arange(half, dtype=jnp.float32) * 2.0 / head_dim))
    angles = position.astype(jnp.float32)[:, None] * frequency[None, :]
    cosine = jnp.cos(angles)[:, None, :]
    sine = jnp.sin(angles)[:, None, :]
    first = values[..., :half]
    second = values[..., half:]
    return jnp.concatenate(
        [first * cosine - second * sine, second * cosine + first * sine], axis=-1
    )


def pick_kernel(count, spots_ref, kv_ref, out_ref):
    base = pl.program_id(1) * count

    def step(i, carry):
        out_ref[0, 0, i] = kv_ref[0, spots_ref[base + i]]
        return carry

    lax.fori_loop(0, count, step, 0, unroll=8)


def pick_pages(kv_old, spots, sections):
    heads, pool, page, width = kv_old.shape
    count = spots.shape[0] // sections
    return pl.pallas_call(
        functools.partial(pick_kernel, count),
        out_shape=jax.ShapeDtypeStruct((sections, heads, count, page, width), kv_old.dtype),
        grid_spec=pltpu.PrefetchScalarGridSpec(
            num_scalar_prefetch=1,
            grid=(heads, sections),
            in_specs=[pl.BlockSpec((1, pool, page, width), lambda h, s, spots: (h, 0, 0, 0))],
            out_specs=pl.BlockSpec(
                (1, 1, count, page, width), lambda h, s, spots: (s, h, 0, 0, 0)
            ),
        ),
        compiler_params=pltpu.CompilerParams(vmem_limit_bytes=VMEM_LIMIT),
        name="pick_pages",
    )(spots, kv_old)


def exchange_kernel(
    sections,
    tensors,
    local_heads,
    repeats,
    kept,
    normed_ref,
    wq_ref,
    pages_ref,
    wkv_ref,
    part_ref,
    arrived_ref,
    wkv_new_ref,
    wq_new_ref,
    stage_ref,
    stage_wkv_ref,
    late_ref,
    held,
    spread,
    made,
    part_in,
    page_send,
    page_recv,
    wkv_send,
    wkv_recv,
    local_sem,
    own_send,
    relay_send,
    wq_recv,
    stage_send,
    stage_recv,
    wkv_own_send,
    wkv_relay_send,
    wkv_stage_recv,
    help_send,
    help_recv,
):
    me = lax.axis_index("section")
    mine = lax.axis_index("tensor")
    depth, columns = wq_ref.shape
    width = wkv_new_ref.shape[1]
    block = wkv_ref.shape[0]
    late_rows = late_ref.shape[0]
    chunks = own_send.shape[1]
    chunk = depth // chunks
    last = sections - 1
    onward = (me < last, me > 0)
    next_to = (me + 1, me - 1)
    feeds = (me == last - 1, me == 1)
    fed = (me == last, me == 0)

    def wq_rows(owner, i):
        return wq_new_ref.at[pl.ds(pl.multiple_of(owner * depth + i * chunk, 16), chunk), :]

    def own_copy(side, i):
        return pltpu.make_async_remote_copy(
            wq_ref.at[pl.ds(pl.multiple_of(i * chunk, 16), chunk), :],
            wq_rows(me, i),
            own_send.at[side, i],
            wq_recv.at[me, i],
            device_id=(next_to[side], mine),
            device_id_type=MESH,
        )

    def relay_copy(owner, side, i):
        return pltpu.make_async_remote_copy(
            wq_rows(owner, i),
            wq_rows(owner, i),
            relay_send.at[owner, i],
            wq_recv.at[owner, i],
            device_id=(next_to[side], mine),
            device_id_type=MESH,
        )

    def each_chunk(act, first=0, end=chunks):
        def run(i, carry):
            act(i)
            return carry

        lax.fori_loop(first, end, run, 0)

    def goes(side, i):
        return jnp.logical_and(
            onward[side], jnp.logical_or(jnp.logical_not(feeds[side]), i < kept)
        )

    def send_own(i):
        for side in range(2):
            pl.when(goes(side, i))(lambda: own_copy(side, i).start())

    def owner_of(side, step):
        return (me - step, me + step)[side]

    def real(side, step):
        return (me - step >= 0, me + step < sections)[side]

    def stage_copy(origin, other, step):
        return pltpu.make_async_remote_copy(
            pages_ref.at[other],
            stage_ref.at[origin],
            stage_send.at[step],
            stage_recv.at[origin],
            device_id=(other, mine),
            device_id_type=MESH,
        )

    part_rows = block // PIECES

    def wkv_own_copy(side, p):
        return pltpu.make_async_remote_copy(
            wkv_ref.at[pl.ds(p * part_rows, part_rows), :],
            stage_wkv_ref.at[me, pl.ds(p * part_rows, part_rows), :],
            wkv_own_send.at[side, p],
            wkv_stage_recv.at[me, p],
            device_id=(next_to[side], mine),
            device_id_type=MESH,
        )

    def wkv_relay_copy(owner, side, p):
        here = stage_wkv_ref.at[owner, pl.ds(p * part_rows, part_rows), :]
        return pltpu.make_async_remote_copy(
            here,
            here,
            wkv_relay_send.at[owner, p],
            wkv_stage_recv.at[owner, p],
            device_id=(next_to[side], mine),
            device_id_type=MESH,
        )

    def page_copy(step, head, copy):
        slot = (step * local_heads + head) * repeats + copy
        other = lax.rem(me + step, sections)
        target = (other * local_heads + head) * repeats + copy
        source = pages_ref.at[me, head] if step == 0 else stage_ref.at[other, head]
        here = (source, arrived_ref.at[mine])
        remote = pltpu.make_async_remote_copy(
            *here,
            page_send.at[slot],
            page_recv.at[mine],
            device_id=(me, target),
            device_id_type=MESH,
        )
        return target, remote, pltpu.make_async_copy(*here, local_sem.at[0])

    def wkv_copy(step, head, copy):
        slot = (step * local_heads + head) * repeats + copy
        other = lax.rem(me + step, sections)
        target = (other * local_heads + head) * repeats + copy
        here = (
            (wkv_ref if step == 0 else stage_wkv_ref.at[other]).at[:, pl.ds(head * width, width)],
            wkv_new_ref.at[pl.ds(pl.multiple_of(mine * block, 128), block), :],
        )
        remote = pltpu.make_async_remote_copy(
            *here,
            wkv_send.at[slot],
            wkv_recv.at[mine],
            device_id=(me, target),
            device_id_type=MESH,
        )
        return target, remote, pltpu.make_async_copy(*here, local_sem.at[1])

    def begin(make, step):
        for head in range(local_heads):
            for copy in range(repeats):
                target, remote, local = make(step, head, copy)
                pl.when(target != mine)(remote.start)
                pl.when(target == mine)(local.start)

    def spread_copy(side):
        feeder = (last - 1, 1)[side]
        start = pl.multiple_of(feeder * depth + depth - late_rows, 128)
        return pltpu.make_async_remote_copy(
            normed_ref.at[:, pl.ds(start, late_rows)],
            spread.at[side],
            help_send.at[0],
            help_recv.at[side],
            device_id=(feeder, mine),
            device_id_type=MESH,
        )

    def part_copy(side):
        return pltpu.make_async_remote_copy(
            made.at[side],
            part_in,
            help_send.at[1 + side],
            help_recv.at[2],
            device_id=((last, 0)[side], mine),
            device_id_type=MESH,
        )

    for side in range(2):
        for p in range(PIECES):
            pl.when(onward[side])(lambda: wkv_own_copy(side, p).start())
        pl.when(fed[side])(lambda: spread_copy(side).start())
    begin(wkv_copy, 0)
    begin(page_copy, 0)
    ahead = min(kept, CHUNKS * 3 // 8)
    each_chunk(send_own, 0, ahead)
    for step in range(sections - 1, 0, -1):
        for side in range(2):
            pl.when(real(side, step))(
                lambda: stage_copy(
                    me, owner_of(side, step), step if side else sections - step
                ).start()
            )
    each_chunk(send_own, ahead)

    take = pltpu.make_async_copy(
        wq_ref.at[pl.ds(depth - late_rows, late_rows), :], held, local_sem.at[2]
    )
    take.start()
    take.wait()
    put = pltpu.make_async_copy(held, late_ref, local_sem.at[3])
    put.start()
    tile = 256
    for side in range(2):

        @pl.when(feeds[side])
        def _():
            spread_copy(side).wait_recv()

            def product(i, carry):
                span = pl.ds(pl.multiple_of(i * tile, tile), tile)
                made[side, :, span] = jnp.dot(
                    spread[side], held[:, span], preferred_element_type=jnp.float32
                )
                return carry

            lax.fori_loop(0, columns // tile, product, 0)
            part_copy(side).start()

    def pass_wkv(step):
        for p in range(PIECES):
            for side in range(2):
                owner = owner_of(side, step)

                @pl.when(real(side, step))
                def _():
                    wkv_relay_copy(owner, side, p).wait_recv()
                    pl.when(onward[side])(lambda: wkv_relay_copy(owner, side, p).start())

        for side in range(2):
            pl.when(real(side, step))(
                lambda: begin(wkv_copy, step if side else sections - step)
            )

    def pass_wq(step, first=0, stop=chunks):
        def pass_on(i):
            for side in range(2):
                owner = owner_of(side, step)
                there = real(side, step)
                if step == 1:
                    there = jnp.logical_and(
                        there, jnp.logical_or(jnp.logical_not(fed[side]), i < kept)
                    )

                @pl.when(there)
                def _():
                    relay_copy(owner, side, i).wait_recv()
                    pl.when(onward[side])(lambda: relay_copy(owner, side, i).start())

        each_chunk(pass_on, first, stop)

    def spread_pages(away, other):
        stage_copy(other, other, away).wait_recv()
        begin(page_copy, away)

    pass_wkv(1)
    pass_wq(1, 0, ahead)
    for step in range(sections - 1, 0, -1):
        for side in range(2):
            pl.when(real(side, step))(
                lambda: spread_pages(
                    step if side else sections - step, owner_of(side, step)
                )
            )
    pass_wq(1, ahead)
    for step in range(2, sections):
        pass_wkv(step)
        if step < last:
            pass_wq(step)

    put.wait()
    for side in range(2):

        @pl.when(fed[side])
        def _():
            spread_copy(side).wait_send()
            part_copy(side).wait_recv()

        pl.when(feeds[side])(lambda: part_copy(side).wait_send())
    end = jnp.logical_or(fed[0], fed[1])

    @pl.when(end)
    def _():
        part_ref[...] = part_in[...]

    @pl.when(jnp.logical_not(end))
    def _():
        part_ref[...] = jnp.zeros_like(part_ref)

    def sent(i):
        for side in range(2):
            pl.when(goes(side, i))(lambda: own_copy(side, i).wait_send())
            for step in range(1, sections):
                pl.when(jnp.logical_and(real(side, step), onward[side]))(
                    lambda: relay_copy(owner_of(side, step), side, i).wait_send()
                )

    each_chunk(sent)
    for side in range(2):
        for p in range(PIECES):
            pl.when(onward[side])(lambda: wkv_own_copy(side, p).wait_send())
            for step in range(1, sections):
                pl.when(jnp.logical_and(real(side, step), onward[side]))(
                    lambda: wkv_relay_copy(owner_of(side, step), side, p).wait_send()
                )
    for step in range(1, sections):
        stage_copy(me, lax.rem(me + step, sections), step).wait_send()
    for make in (page_copy, wkv_copy):
        for step in range(sections):
            for head in range(local_heads):
                for copy in range(repeats):
                    target, remote, local = make(step, head, copy)
                    pl.when(target != mine)(remote.wait_send)
                    pl.when(target == mine)(local.wait)
    for origin in range(tensors):
        pages_in = pltpu.make_async_remote_copy(
            pages_ref.at[0, 0],
            arrived_ref.at[origin],
            page_send.at[0],
            page_recv.at[origin],
            device_id=(me, origin),
            device_id_type=MESH,
        )
        wkv_in = pltpu.make_async_remote_copy(
            wkv_ref.at[:, pl.ds(0, width)],
            wkv_new_ref.at[pl.ds(origin * block, block), :],
            wkv_send.at[0],
            wkv_recv.at[origin],
            device_id=(me, origin),
            device_id_type=MESH,
        )
        outside = mine != origin
        pl.when(outside)(pages_in.wait_recv)
        pl.when(outside)(wkv_in.wait_recv)
    if last > 1:
        pass_wq(last)


def exchange(normed, wq_old, pages, wkv_old, sections, tensors, repeats):
    rows = normed.shape[0]
    depth, columns = wq_old.shape
    local_heads = pages.shape[1]
    width = pages.shape[4]
    copies = sections * local_heads * repeats
    tiles, early, late = split(depth)
    late_rows = late * UNIT
    kept = (tiles - early - late) * UNIT * CHUNKS // depth
    dma = pltpu.SemaphoreType.DMA
    vmem = pl.BlockSpec(memory_space=pltpu.VMEM)
    hbm = pl.BlockSpec(memory_space=pl.ANY)
    return pl.pallas_call(
        functools.partial(
            exchange_kernel, sections, tensors, local_heads, repeats, kept
        ),
        out_shape=(
            jax.ShapeDtypeStruct((rows, columns), jnp.float32),
            jax.ShapeDtypeStruct((tensors,) + pages.shape[2:], pages.dtype),
            jax.ShapeDtypeStruct((wkv_old.shape[0] * tensors, width), wkv_old.dtype),
            jax.ShapeDtypeStruct((depth * sections, columns), wq_old.dtype),
            jax.ShapeDtypeStruct(pages.shape, pages.dtype),
            jax.ShapeDtypeStruct((sections,) + wkv_old.shape, wkv_old.dtype),
            jax.ShapeDtypeStruct((late_rows, columns), wq_old.dtype),
        ),
        in_specs=[vmem, hbm, hbm, hbm],
        out_specs=(vmem, hbm, hbm, hbm, hbm, hbm, hbm),
        scratch_shapes=[
            pltpu.VMEM((late_rows, columns), wq_old.dtype),
            pltpu.VMEM((2, rows, late_rows), normed.dtype),
            pltpu.VMEM((2, rows, columns), jnp.float32),
            pltpu.VMEM((rows, columns), jnp.float32),
            dma((copies,)),
            dma((tensors,)),
            dma((copies,)),
            dma((tensors,)),
            dma((4,)),
            dma((2, CHUNKS)),
            dma((sections, CHUNKS)),
            dma((sections, CHUNKS)),
            dma((sections,)),
            dma((sections,)),
            dma((2, PIECES)),
            dma((sections, PIECES)),
            dma((sections, PIECES)),
            dma((3,)),
            dma((3,)),
        ],
        compiler_params=pltpu.CompilerParams(
            has_side_effects=True, vmem_limit_bytes=VMEM_LIMIT
        ),
        cost_estimate=pl.CostEstimate(
            flops=4 * rows * late_rows * columns,
            bytes_accessed=400 * 2**20,
            transcendentals=0,
        ),
        name="exchange",
    )(normed, wq_old, pages, wkv_old)


def gather_kernel(
    sections,
    tiles,
    first,
    last,
    pair,
    me_ref,
    normed_ref,
    part_ref,
    own_ref,
    far_ref,
    early_ref,
    wkv_ref,
    out_ref,
    query_ref,
    wkv_out_ref,
    fresh_ref,
    total,
    fresh,
):
    i = pl.program_id(0)
    me = me_ref[0]
    owner = i // (tiles // pair)
    tile = UNIT
    mine = owner == me
    fed = jnp.logical_or(
        jnp.logical_and(me == sections - 1, owner == sections - 2),
        jnp.logical_and(me == 0, owner == 1),
    )

    @pl.when(i == 0)
    def _():
        total[...] = part_ref[...]
        fresh[...] = jnp.zeros_like(fresh)

    def keep(ref, rows, at):
        out_ref[pl.ds(at * tile, tile), :] = ref[rows, :]

    for at in range(pair):
        k = (i % (tiles // pair)) * pair + at
        rows = pl.ds(at * tile, tile)
        early = jnp.logical_and(fed, jnp.logical_and(k >= first, k < last))
        late = jnp.logical_and(fed, k >= last)
        start = jnp.clip(k - first, 0, last - first - 1) * tile
        other = jnp.logical_or(mine, jnp.logical_or(early, late))
        pl.when(mine)(lambda: keep(own_ref, rows, at))
        pl.when(early)(
            lambda: keep(early_ref, pl.ds(pl.multiple_of(start, UNIT), tile), at)
        )
        pl.when(jnp.logical_not(other))(lambda: keep(far_ref, rows, at))

        @pl.when(late)
        def _():
            out_ref[rows, :] = jnp.zeros((tile, out_ref.shape[1]), out_ref.dtype)

    span = pl.ds(pl.multiple_of(i * pair * tile, UNIT), pair * tile)
    features = normed_ref[:, span]
    total[...] += jnp.dot(features, out_ref[...], preferred_element_type=jnp.float32)
    wkv_out_ref[...] = wkv_ref[...]
    fresh[...] += jnp.dot(features, wkv_ref[...], preferred_element_type=jnp.float32)

    @pl.when(i == pl.num_programs(0) - 1)
    def _():
        query_ref[...] = total[...]
        fresh_ref[...] = fresh[...]


def gather(me, normed, part, wq_old, far, early, wkv, sections):
    rows, total_depth = normed.shape
    depth, columns = wq_old.shape
    tiles, early_tiles, late_tiles = split(depth)
    pair = min(PAIR, tiles)
    steps = tiles // pair
    tile = pair * UNIT
    width = wkv.shape[1]

    def own_at(i, me):
        return (jnp.clip(i - me[0] * steps, 0, steps - 1), 0)

    def far_at(i, me):
        own = i // steps == me[0]
        return (jnp.where(own, jnp.maximum(me[0] * steps - 1, 0), i), 0)

    return pl.pallas_call(
        functools.partial(
            gather_kernel,
            sections,
            tiles,
            tiles - early_tiles - late_tiles,
            tiles - late_tiles,
            pair,
        ),
        out_shape=(
            jax.ShapeDtypeStruct((total_depth, columns), wq_old.dtype),
            jax.ShapeDtypeStruct((rows, columns), jnp.float32),
            jax.ShapeDtypeStruct(wkv.shape, wkv.dtype),
            jax.ShapeDtypeStruct((rows, width), jnp.float32),
        ),
        grid_spec=pltpu.PrefetchScalarGridSpec(
            num_scalar_prefetch=1,
            grid=(sections * steps,),
            in_specs=[
                pl.BlockSpec((rows, total_depth), lambda i, me: (0, 0)),
                pl.BlockSpec((rows, columns), lambda i, me: (0, 0)),
                pl.BlockSpec((tile, columns), own_at),
                pl.BlockSpec((tile, columns), far_at),
                pl.BlockSpec(early.shape, lambda i, me: (0, 0)),
                pl.BlockSpec((tile, width), lambda i, me: (i, 0)),
            ],
            out_specs=(
                pl.BlockSpec((tile, columns), lambda i, me: (i, 0)),
                pl.BlockSpec((rows, columns), lambda i, me: (0, 0)),
                pl.BlockSpec((tile, width), lambda i, me: (i, 0)),
                pl.BlockSpec((rows, width), lambda i, me: (0, 0)),
            ),
            scratch_shapes=[
                pltpu.VMEM((rows, columns), jnp.float32),
                pltpu.VMEM((rows, width), jnp.float32),
            ],
        ),
        cost_estimate=pl.CostEstimate(
            flops=2 * rows * total_depth * columns,
            bytes_accessed=4 * total_depth * columns,
            transcendentals=0,
        ),
        compiler_params=pltpu.CompilerParams(vmem_limit_bytes=VMEM_LIMIT),
        name="gather_query",
    )(me, normed, part, wq_old, far, early, wkv)


def place_kernel(sections, depth, late_ref, held_ref, out_ref, done):
    me = lax.axis_index("section")
    pieces = done.shape[0]
    piece = late_ref.shape[0] // pieces
    feeder = jnp.where(me == 0, 1, sections - 2)
    start = feeder * depth + depth - late_ref.shape[0]

    def write(p):
        return pltpu.make_async_copy(
            late_ref.at[pl.ds(p * piece, piece), :],
            out_ref.at[pl.ds(pl.multiple_of(start + p * piece, 16), piece), :],
            done.at[p],
        )

    @pl.when(jnp.logical_or(me == 0, me == sections - 1))
    def _():
        for p in range(pieces):
            write(p).start()
        for p in range(pieces):
            write(p).wait()


def place_late(late, wq_new, sections):
    depth = wq_new.shape[0] // sections
    hbm = pl.BlockSpec(memory_space=pl.ANY)
    return pl.pallas_call(
        functools.partial(place_kernel, sections, depth),
        out_shape=jax.ShapeDtypeStruct(wq_new.shape, wq_new.dtype),
        in_specs=[pl.BlockSpec(memory_space=pltpu.VMEM), hbm],
        out_specs=hbm,
        scratch_shapes=[pltpu.SemaphoreType.DMA((2,))],
        input_output_aliases={1: 0},
        cost_estimate=pl.CostEstimate(
            flops=1024, bytes_accessed=4 * late.size, transcendentals=0
        ),
        compiler_params=pltpu.CompilerParams(vmem_limit_bytes=16 * 2**20),
        name="place_late",
    )(late, wq_new)


def take_kernel(start, from_ref, out_ref, done):
    copy = pltpu.make_async_copy(from_ref.at[pl.ds(start, out_ref.shape[0]), :], out_ref, done)
    copy.start()
    copy.wait()


def take_rows(array, start, rows):
    return pl.pallas_call(
        functools.partial(take_kernel, start),
        out_shape=jax.ShapeDtypeStruct((rows, array.shape[1]), array.dtype),
        in_specs=[pl.BlockSpec(memory_space=pl.ANY)],
        out_specs=pl.BlockSpec(memory_space=pltpu.VMEM),
        scratch_shapes=[pltpu.SemaphoreType.DMA],
        compiler_params=pltpu.CompilerParams(vmem_limit_bytes=VMEM_LIMIT),
        name="take_rows",
    )(array)


def attend_kernel(
    pages_of, together, page, head_dim, block_ref, spot_ref, length_ref, in_ref, fresh_ref, query_ref, cache_ref, context_ref, mixed
):
    step = pl.program_id(0)

    def order(j, carry):
        start = pl.multiple_of(j * page, page)
        for r in range(together):
            at = (step * together + r) * pages_of + j
            cache_ref[r, pl.ds(start, page), :] = in_ref[block_ref[at], r, spot_ref[at]]
        return carry

    lax.fori_loop(0, pages_of, order, 0, unroll=8)
    for r in range(together):
        length = length_ref[step * together + r]
        start = pl.multiple_of(lax.div(length, page) * page, page)
        held = cache_ref[r, pl.ds(start, page), :]
        row = lax.broadcasted_iota(jnp.int32, held.shape, 0)
        fresh = jnp.broadcast_to(fresh_ref[r].astype(jnp.float32), held.shape)
        cache_ref[r, pl.ds(start, page), :] = jnp.where(
            row == lax.rem(length, page), fresh, held.astype(jnp.float32)
        ).astype(held.dtype)
    scores = [
        lax.dot_general(
            query_ref[r],
            cache_ref[r, :, :head_dim],
            (((1,), (1,)), ((), ())),
            preferred_element_type=jnp.float32,
        )
        * head_dim ** (-0.5)
        for r in range(together)
    ]
    seen = [
        lax.broadcasted_iota(jnp.int32, scores[r].shape, 1) <= length_ref[step * together + r]
        for r in range(together)
    ]
    peak = [
        jnp.max(jnp.where(seen[r], scores[r], -jnp.inf), axis=1, keepdims=True)
        for r in range(together)
    ]
    weights = [jnp.where(seen[r], jnp.exp(scores[r] - peak[r]), 0.0) for r in range(together)]
    sums = [jnp.sum(weights[r], axis=1, keepdims=True) for r in range(together)]
    probs = [(weights[r] / sums[r]).astype(jnp.bfloat16) for r in range(together)]
    for r in range(together):
        mixed[step * together + r] = jnp.dot(
            probs[r], cache_ref[r, :, head_dim:], preferred_element_type=jnp.float32
        )

    @pl.when(step == pl.num_programs(0) - 1)
    def _():
        for head in range(mixed.shape[1]):
            context_ref[:, pl.ds(head * head_dim, head_dim)] = mixed[:, head].astype(
                context_ref.dtype
            )


def attend(arrived, block, spot, lengths, fresh, query, head_dim):
    blocks, rows, per_block, page, width = arrived.shape
    pages_of = blocks * per_block
    heads = query.shape[1]
    together = next(n for n in (TOGETHER, 2, 1) if rows % n == 0)
    return pl.pallas_call(
        functools.partial(attend_kernel, pages_of, together, page, head_dim),
        out_shape=(
            jax.ShapeDtypeStruct((rows, pages_of * page, width), arrived.dtype),
            jax.ShapeDtypeStruct((rows, heads * head_dim), jnp.bfloat16),
        ),
        grid_spec=pltpu.PrefetchScalarGridSpec(
            num_scalar_prefetch=3,
            grid=(rows // together,),
            in_specs=[
                pl.BlockSpec(
                    (blocks, together, per_block, page, width), lambda r, *_: (0, r, 0, 0, 0)
                ),
                pl.BlockSpec((together, 1, width), lambda r, *_: (r, 0, 0)),
                pl.BlockSpec((together, heads, head_dim), lambda r, *_: (r, 0, 0)),
            ],
            out_specs=(
                pl.BlockSpec((together, pages_of * page, width), lambda r, *_: (r, 0, 0)),
                pl.BlockSpec((rows, heads * head_dim), lambda r, *_: (0, 0)),
            ),
            scratch_shapes=[pltpu.VMEM((rows, heads, head_dim), jnp.float32)],
        ),
        cost_estimate=pl.CostEstimate(
            flops=4 * rows * heads * pages_of * page * head_dim,
            bytes_accessed=4 * arrived.size,
            transcendentals=rows * heads * pages_of * page,
        ),
        compiler_params=pltpu.CompilerParams(vmem_limit_bytes=VMEM_LIMIT),
        name="attend",
    )(block.reshape(-1), spot.reshape(-1), lengths, arrived, fresh[:, None, :], query)


def work(hidden_state, norm_gain, wq_old, wkv_old, kv_old, page_table, lengths):
    sections = lax.axis_size("section")
    tensors = lax.axis_size("tensor")
    section_id = lax.axis_index("section")
    tensor_id = lax.axis_index("tensor")
    rows = hidden_state.shape[0]
    head_dim = HEAD_DIM
    width = 2 * head_dim
    repeats = tensors // KV_HEADS
    queries_here = wq_old.shape[1] // head_dim
    pool_dev = kv_old.shape[1]
    page = kv_old.shape[2]
    per_block = page_table.shape[1] // tensors
    widened = hidden_state.astype(jnp.float32)
    scale = lax.rsqrt(jnp.mean(widened * widened, axis=1, keepdims=True) + EPSILON)
    normed = (widened * scale * norm_gain[None, :]).astype(jnp.bfloat16)
    owner = page_table // pool_dev
    blocks = jnp.arange(tensors, dtype=jnp.int32)
    onehot = (owner[:, :, None] == blocks[None, None, :]).astype(jnp.int32)
    ranks = jnp.sum((jnp.cumsum(onehot, axis=1) - 1) * onehot, axis=2)
    mine = owner == tensor_id
    wanted = ranks[:, :, None] == jnp.arange(per_block, dtype=jnp.int32)[None, None, :]
    picks = (mine[:, :, None] & wanted).astype(jnp.int32)
    spots = jnp.sum(picks * (page_table % pool_dev)[:, :, None], axis=1)
    pages = pick_pages(kv_old, spots.reshape(-1), sections)
    depth = wq_old.shape[0]
    ends = sorted({(sections - 2, sections - 1), (1, 0)})
    tiles, early_tiles, late_tiles = split(depth)
    early = take_rows(
        wq_old, (tiles - early_tiles - late_tiles) * UNIT, early_tiles * UNIT
    )
    early = lax.ppermute(early, "section", ends)
    part, arrived, wkv_far, far, _, _, late = exchange(
        normed, wq_old, pages, wkv_old, sections, tensors, repeats
    )
    late = lax.ppermute(late, "section", ends)
    me = jnp.full((1,), section_id, jnp.int32)
    wq_new, query, wkv_new, fresh = gather(
        me, normed, part, wq_old, far, early, wkv_far, sections
    )
    arrived = arrived.reshape(tensors, rows, per_block, page, width)
    block = lax.dynamic_slice_in_dim(owner, section_id * rows, rows, 0)
    spot = lax.dynamic_slice_in_dim(ranks, section_id * rows, rows, 0)
    my_lengths = lax.dynamic_slice_in_dim(lengths, section_id * rows, rows, 0)
    fresh_key = rotate(fresh[:, None, :head_dim], my_lengths, head_dim)[:, 0]
    fresh = jnp.concatenate([fresh_key, fresh[:, head_dim:]], axis=1).astype(jnp.bfloat16)
    query = rotate(query.reshape(rows, queries_here, head_dim), my_lengths, head_dim).astype(
        jnp.bfloat16
    )
    cache, context = attend(arrived, block, spot, my_lengths, fresh, query, head_dim)
    wq_new = place_late(late, wq_new, sections)
    return (context, cache[:, None], wq_new, wkv_new)


def solution(mesh):
    placed = (
        P("section", None),
        P(),
        P("section", "tensor"),
        P("tensor", "section"),
        P("section", "tensor", None, None),
        P(),
        P(),
    )
    return jax.shard_map(
        work,
        mesh=mesh,
        in_specs=placed,
        out_specs=(
            P("section", "tensor"),
            P("section", "tensor", None, None),
            P(None, "tensor"),
            P(None, "tensor"),
        ),
        check_vma=False,
    )
```

```python
import functools

import jax
import jax.numpy as jnp
from jax import lax
from jax.experimental import pallas as pl
from jax.experimental.pallas import tpu as pltpu
from jax.sharding import PartitionSpec as P


KV_HEADS = 8
HEAD_DIM = 128


EPSILON = 1e-05
ROPE_BASE = 500000.0
MESH = pl.DeviceIdType.MESH
CHUNKS = 16
PIECES = 4
STAGGER = 3
UNIT = 128
EARLY = 4
LATE = 7
PAIR = 8
TOGETHER = 4
VMEM_LIMIT = 60 * 2**20


def split(depth):
    tiles = depth // UNIT
    return tiles, max(1, tiles * EARLY // 16), max(1, tiles * LATE // 16)


def rotate(values, position, head_dim):
    half = head_dim // 2
    frequency = ROPE_BASE ** (-(jnp.arange(half, dtype=jnp.float32) * 2.0 / head_dim))
    angles = position.astype(jnp.float32)[:, None] * frequency[None, :]
    cosine = jnp.cos(angles)[:, None, :]
    sine = jnp.sin(angles)[:, None, :]
    first = values[..., :half]
    second = values[..., half:]
    return jnp.concatenate(
        [first * cosine - second * sine, second * cosine + first * sine], axis=-1
    )


def pick_kernel(count, spots_ref, kv_ref, out_ref):
    base = pl.program_id(1) * count

    def step(i, carry):
        out_ref[0, 0, i] = kv_ref[0, spots_ref[base + i]]
        return carry

    lax.fori_loop(0, count, step, 0, unroll=8)


def pick_pages(kv_old, spots, sections):
    heads, pool, page, width = kv_old.shape
    count = spots.shape[0] // sections
    return pl.pallas_call(
        functools.partial(pick_kernel, count),
        out_shape=jax.ShapeDtypeStruct((sections, heads, count, page, width), kv_old.dtype),
        grid_spec=pltpu.PrefetchScalarGridSpec(
            num_scalar_prefetch=1,
            grid=(heads, sections),
            in_specs=[pl.BlockSpec((1, pool, page, width), lambda h, s, spots: (h, 0, 0, 0))],
            out_specs=pl.BlockSpec(
                (1, 1, count, page, width), lambda h, s, spots: (s, h, 0, 0, 0)
            ),
        ),
        compiler_params=pltpu.CompilerParams(vmem_limit_bytes=VMEM_LIMIT),
        name="pick_pages",
    )(spots, kv_old)


def exchange_kernel(
    sections,
    tensors,
    local_heads,
    repeats,
    kept,
    normed_ref,
    wq_ref,
    pages_ref,
    wkv_ref,
    part_ref,
    arrived_ref,
    wkv_new_ref,
    wq_new_ref,
    stage_ref,
    stage_wkv_ref,
    late_ref,
    held,
    spread,
    made,
    part_in,
    page_send,
    page_recv,
    wkv_send,
    wkv_recv,
    local_sem,
    own_send,
    relay_send,
    wq_recv,
    stage_send,
    stage_recv,
    wkv_own_send,
    wkv_relay_send,
    wkv_stage_recv,
    help_send,
    help_recv,
    turn,
):
    me = lax.axis_index("section")
    mine = lax.axis_index("tensor")
    depth, columns = wq_ref.shape
    width = wkv_new_ref.shape[1]
    block = wkv_ref.shape[0]
    late_rows = late_ref.shape[0]
    chunks = own_send.shape[1]
    chunk = depth // chunks
    last = sections - 1
    onward = (me < last, me > 0)
    next_to = (me + 1, me - 1)
    feeds = (me == last - 1, me == 1)
    fed = (me == last, me == 0)

    def wq_rows(owner, i):
        return wq_new_ref.at[pl.ds(pl.multiple_of(owner * depth + i * chunk, 16), chunk), :]

    def own_copy(side, i):
        return pltpu.make_async_remote_copy(
            wq_ref.at[pl.ds(pl.multiple_of(i * chunk, 16), chunk), :],
            wq_rows(me, i),
            own_send.at[side, i],
            wq_recv.at[me, i],
            device_id=(next_to[side], mine),
            device_id_type=MESH,
        )

    def relay_copy(owner, side, i):
        return pltpu.make_async_remote_copy(
            wq_rows(owner, i),
            wq_rows(owner, i),
            relay_send.at[owner, i],
            wq_recv.at[owner, i],
            device_id=(next_to[side], mine),
            device_id_type=MESH,
        )

    def each_chunk(act, first=0, end=chunks):
        def run(i, carry):
            act(i)
            return carry

        lax.fori_loop(first, end, run, 0)

    def goes(side, i):
        return jnp.logical_and(
            onward[side], jnp.logical_or(jnp.logical_not(feeds[side]), i < kept)
        )

    def send_own(i):
        for side in range(2):
            pl.when(goes(side, i))(lambda: own_copy(side, i).start())

    def owner_of(side, step):
        return (me - step, me + step)[side]

    def real(side, step):
        return (me - step >= 0, me + step < sections)[side]

    def stage_copy(origin, other, step):
        return pltpu.make_async_remote_copy(
            pages_ref.at[other],
            stage_ref.at[origin],
            stage_send.at[step],
            stage_recv.at[origin],
            device_id=(other, mine),
            device_id_type=MESH,
        )

    part_rows = block // PIECES

    def wkv_own_copy(side, p):
        return pltpu.make_async_remote_copy(
            wkv_ref.at[pl.ds(p * part_rows, part_rows), :],
            stage_wkv_ref.at[me, pl.ds(p * part_rows, part_rows), :],
            wkv_own_send.at[side, p],
            wkv_stage_recv.at[me, p],
            device_id=(next_to[side], mine),
            device_id_type=MESH,
        )

    def wkv_relay_copy(owner, side, p):
        here = stage_wkv_ref.at[owner, pl.ds(p * part_rows, part_rows), :]
        return pltpu.make_async_remote_copy(
            here,
            here,
            wkv_relay_send.at[owner, p],
            wkv_stage_recv.at[owner, p],
            device_id=(next_to[side], mine),
            device_id_type=MESH,
        )

    def page_copy(step, head, copy):
        slot = (step * local_heads + head) * repeats + copy
        other = lax.rem(me + step, sections)
        target = (other * local_heads + head) * repeats + copy
        source = pages_ref.at[me, head] if step == 0 else stage_ref.at[other, head]
        here = (source, arrived_ref.at[mine])
        remote = pltpu.make_async_remote_copy(
            *here,
            page_send.at[slot],
            page_recv.at[mine],
            device_id=(me, target),
            device_id_type=MESH,
        )
        return target, remote, pltpu.make_async_copy(*here, local_sem.at[0])

    def wkv_copy(step, head, copy):
        slot = (step * local_heads + head) * repeats + copy
        other = lax.rem(me + step, sections)
        target = (other * local_heads + head) * repeats + copy
        here = (
            (wkv_ref if step == 0 else stage_wkv_ref.at[other]).at[:, pl.ds(head * width, width)],
            wkv_new_ref.at[pl.ds(pl.multiple_of(mine * block, 128), block), :],
        )
        remote = pltpu.make_async_remote_copy(
            *here,
            wkv_send.at[slot],
            wkv_recv.at[mine],
            device_id=(me, target),
            device_id_type=MESH,
        )
        return target, remote, pltpu.make_async_copy(*here, local_sem.at[1])

    def begin(make, step):
        for head in range(local_heads):
            for copy in range(repeats):
                target, remote, local = make(step, head, copy)
                pl.when(target != mine)(remote.start)
                pl.when(target == mine)(local.start)

    def spread_copy(side):
        feeder = (last - 1, 1)[side]
        start = pl.multiple_of(feeder * depth + depth - late_rows, 128)
        return pltpu.make_async_remote_copy(
            normed_ref.at[:, pl.ds(start, late_rows)],
            spread.at[side],
            help_send.at[0],
            help_recv.at[side],
            device_id=(feeder, mine),
            device_id_type=MESH,
        )

    def part_copy(side):
        return pltpu.make_async_remote_copy(
            made.at[side],
            part_in,
            help_send.at[1 + side],
            help_recv.at[2],
            device_id=((last, 0)[side], mine),
            device_id_type=MESH,
        )

    for side in range(2):
        pl.when(fed[side])(lambda: spread_copy(side).start())
    begin(wkv_copy, 0)
    begin(page_copy, 0)
    second = lax.rem(mine, 2) == 1
    pl.when(second)(lambda: pl.semaphore_wait(turn, 1))
    for side in range(2):
        for p in range(PIECES):
            pl.when(onward[side])(lambda: wkv_own_copy(side, p).start())
    ahead = CHUNKS * 3 // 8
    each_chunk(send_own, 0, ahead)
    for step in range(sections - 1, 0, -1):
        for side in range(2):
            pl.when(real(side, step))(
                lambda: stage_copy(
                    me, owner_of(side, step), step if side else sections - step
                ).start()
            )
    each_chunk(send_own, ahead)

    @pl.when(jnp.logical_not(second))
    def _():
        for side in range(2):
            for p in range(STAGGER):
                pl.when(onward[side])(lambda: wkv_own_copy(side, p).wait_send())
        pl.semaphore_signal(turn, 1, device_id=(me, mine + 1), device_id_type=MESH)

    take = pltpu.make_async_copy(
        wq_ref.at[pl.ds(depth - late_rows, late_rows), :], held, local_sem.at[2]
    )
    take.start()
    take.wait()
    put = pltpu.make_async_copy(held, late_ref, local_sem.at[3])
    put.start()
    tile = 256
    for side in range(2):

        @pl.when(feeds[side])
        def _():
            spread_copy(side).wait_recv()

            def product(i, carry):
                span = pl.ds(pl.multiple_of(i * tile, tile), tile)
                made[side, :, span] = jnp.dot(
                    spread[side], held[:, span], preferred_element_type=jnp.float32
                )
                return carry

            lax.fori_loop(0, columns // tile, product, 0)
            part_copy(side).start()

    def pass_wkv(step):
        for p in range(PIECES):
            for side in range(2):
                owner = owner_of(side, step)

                @pl.when(real(side, step))
                def _():
                    wkv_relay_copy(owner, side, p).wait_recv()
                    pl.when(onward[side])(lambda: wkv_relay_copy(owner, side, p).start())

        for side in range(2):
            pl.when(real(side, step))(
                lambda: begin(wkv_copy, step if side else sections - step)
            )

    def pass_wq(step, first=0, stop=chunks):
        def pass_on(i):
            for side in range(2):
                owner = owner_of(side, step)
                there = real(side, step)
                if step == 1:
                    there = jnp.logical_and(
                        there, jnp.logical_or(jnp.logical_not(fed[side]), i < kept)
                    )

                @pl.when(there)
                def _():
                    relay_copy(owner, side, i).wait_recv()
                    pl.when(onward[side])(lambda: relay_copy(owner, side, i).start())

        each_chunk(pass_on, first, stop)

    def spread_pages(away, other):
        stage_copy(other, other, away).wait_recv()
        begin(page_copy, away)

    pass_wkv(1)
    pass_wq(1, 0, ahead)
    for step in range(sections - 1, 0, -1):
        for side in range(2):
            pl.when(real(side, step))(
                lambda: spread_pages(
                    step if side else sections - step, owner_of(side, step)
                )
            )
    pass_wq(1, ahead)
    for step in range(2, sections):
        pass_wkv(step)
        if step < last:
            pass_wq(step)

    put.wait()
    for side in range(2):

        @pl.when(fed[side])
        def _():
            spread_copy(side).wait_send()
            part_copy(side).wait_recv()

        pl.when(feeds[side])(lambda: part_copy(side).wait_send())
    end = jnp.logical_or(fed[0], fed[1])

    @pl.when(end)
    def _():
        part_ref[...] = part_in[...]

    @pl.when(jnp.logical_not(end))
    def _():
        part_ref[...] = jnp.zeros_like(part_ref)

    def sent(i):
        for side in range(2):
            pl.when(goes(side, i))(lambda: own_copy(side, i).wait_send())
            for step in range(1, sections):
                pl.when(jnp.logical_and(real(side, step), onward[side]))(
                    lambda: relay_copy(owner_of(side, step), side, i).wait_send()
                )

    each_chunk(sent)
    for side in range(2):
        for p in range(PIECES):
            pl.when(jnp.logical_and(onward[side], jnp.logical_or(second, p >= STAGGER)))(
                lambda: wkv_own_copy(side, p).wait_send()
            )
            for step in range(1, sections):
                pl.when(jnp.logical_and(real(side, step), onward[side]))(
                    lambda: wkv_relay_copy(owner_of(side, step), side, p).wait_send()
                )
    for step in range(1, sections):
        stage_copy(me, lax.rem(me + step, sections), step).wait_send()
    for make in (page_copy, wkv_copy):
        for step in range(sections):
            for head in range(local_heads):
                for copy in range(repeats):
                    target, remote, local = make(step, head, copy)
                    pl.when(target != mine)(remote.wait_send)
                    pl.when(target == mine)(local.wait)
    for origin in range(tensors):
        pages_in = pltpu.make_async_remote_copy(
            pages_ref.at[0, 0],
            arrived_ref.at[origin],
            page_send.at[0],
            page_recv.at[origin],
            device_id=(me, origin),
            device_id_type=MESH,
        )
        wkv_in = pltpu.make_async_remote_copy(
            wkv_ref.at[:, pl.ds(0, width)],
            wkv_new_ref.at[pl.ds(origin * block, block), :],
            wkv_send.at[0],
            wkv_recv.at[origin],
            device_id=(me, origin),
            device_id_type=MESH,
        )
        outside = mine != origin
        pl.when(outside)(pages_in.wait_recv)
        pl.when(outside)(wkv_in.wait_recv)
    if last > 1:
        pass_wq(last)


def exchange(normed, wq_old, pages, wkv_old, sections, tensors, repeats):
    rows = normed.shape[0]
    depth, columns = wq_old.shape
    local_heads = pages.shape[1]
    width = pages.shape[4]
    copies = sections * local_heads * repeats
    tiles, early, late = split(depth)
    late_rows = late * UNIT
    kept = (tiles - early - late) * UNIT * CHUNKS // depth
    dma = pltpu.SemaphoreType.DMA
    vmem = pl.BlockSpec(memory_space=pltpu.VMEM)
    hbm = pl.BlockSpec(memory_space=pl.ANY)
    return pl.pallas_call(
        functools.partial(
            exchange_kernel, sections, tensors, local_heads, repeats, kept
        ),
        out_shape=(
            jax.ShapeDtypeStruct((rows, columns), jnp.float32),
            jax.ShapeDtypeStruct((tensors,) + pages.shape[2:], pages.dtype),
            jax.ShapeDtypeStruct((wkv_old.shape[0] * tensors, width), wkv_old.dtype),
            jax.ShapeDtypeStruct((depth * sections, columns), wq_old.dtype),
            jax.ShapeDtypeStruct(pages.shape, pages.dtype),
            jax.ShapeDtypeStruct((sections,) + wkv_old.shape, wkv_old.dtype),
            jax.ShapeDtypeStruct((late_rows, columns), wq_old.dtype),
        ),
        in_specs=[vmem, hbm, hbm, hbm],
        out_specs=(vmem, hbm, hbm, hbm, hbm, hbm, hbm),
        scratch_shapes=[
            pltpu.VMEM((late_rows, columns), wq_old.dtype),
            pltpu.VMEM((2, rows, late_rows), normed.dtype),
            pltpu.VMEM((2, rows, columns), jnp.float32),
            pltpu.VMEM((rows, columns), jnp.float32),
            dma((copies,)),
            dma((tensors,)),
            dma((copies,)),
            dma((tensors,)),
            dma((4,)),
            dma((2, CHUNKS)),
            dma((sections, CHUNKS)),
            dma((sections, CHUNKS)),
            dma((sections,)),
            dma((sections,)),
            dma((2, PIECES)),
            dma((sections, PIECES)),
            dma((sections, PIECES)),
            dma((3,)),
            dma((3,)),
            pltpu.SemaphoreType.REGULAR,
        ],
        compiler_params=pltpu.CompilerParams(
            has_side_effects=True, vmem_limit_bytes=VMEM_LIMIT
        ),
        cost_estimate=pl.CostEstimate(
            flops=4 * rows * late_rows * columns,
            bytes_accessed=400 * 2**20,
            transcendentals=0,
        ),
        name="exchange",
    )(normed, wq_old, pages, wkv_old)


def gather_kernel(
    sections,
    tiles,
    first,
    last,
    pair,
    me_ref,
    normed_ref,
    part_ref,
    own_ref,
    far_ref,
    early_ref,
    wkv_ref,
    out_ref,
    query_ref,
    wkv_out_ref,
    fresh_ref,
    total,
    fresh,
):
    i = pl.program_id(0)
    me = me_ref[0]
    owner = i // (tiles // pair)
    tile = UNIT
    mine = owner == me
    fed = jnp.logical_or(
        jnp.logical_and(me == sections - 1, owner == sections - 2),
        jnp.logical_and(me == 0, owner == 1),
    )

    @pl.when(i == 0)
    def _():
        total[...] = part_ref[...]
        fresh[...] = jnp.zeros_like(fresh)

    def keep(ref, rows, at):
        out_ref[pl.ds(at * tile, tile), :] = ref[rows, :]

    for at in range(pair):
        k = (i % (tiles // pair)) * pair + at
        rows = pl.ds(at * tile, tile)
        early = jnp.logical_and(fed, jnp.logical_and(k >= first, k < last))
        late = jnp.logical_and(fed, k >= last)
        start = jnp.clip(k - first, 0, last - first - 1) * tile
        other = jnp.logical_or(mine, jnp.logical_or(early, late))
        pl.when(mine)(lambda: keep(own_ref, rows, at))
        pl.when(early)(
            lambda: keep(early_ref, pl.ds(pl.multiple_of(start, UNIT), tile), at)
        )
        pl.when(jnp.logical_not(other))(lambda: keep(far_ref, rows, at))

        @pl.when(late)
        def _():
            out_ref[rows, :] = jnp.zeros((tile, out_ref.shape[1]), out_ref.dtype)

    span = pl.ds(pl.multiple_of(i * pair * tile, UNIT), pair * tile)
    features = normed_ref[:, span]
    total[...] += jnp.dot(features, out_ref[...], preferred_element_type=jnp.float32)
    wkv_out_ref[...] = wkv_ref[...]
    fresh[...] += jnp.dot(features, wkv_ref[...], preferred_element_type=jnp.float32)

    @pl.when(i == pl.num_programs(0) - 1)
    def _():
        query_ref[...] = total[...]
        fresh_ref[...] = fresh[...]


def gather(me, normed, part, wq_old, far, early, wkv, sections):
    rows, total_depth = normed.shape
    depth, columns = wq_old.shape
    tiles, early_tiles, late_tiles = split(depth)
    pair = min(PAIR, tiles)
    steps = tiles // pair
    tile = pair * UNIT
    width = wkv.shape[1]

    def own_at(i, me):
        return (jnp.clip(i - me[0] * steps, 0, steps - 1), 0)

    def far_at(i, me):
        own = i // steps == me[0]
        return (jnp.where(own, jnp.maximum(me[0] * steps - 1, 0), i), 0)

    return pl.pallas_call(
        functools.partial(
            gather_kernel,
            sections,
            tiles,
            tiles - early_tiles - late_tiles,
            tiles - late_tiles,
            pair,
        ),
        out_shape=(
            jax.ShapeDtypeStruct((total_depth, columns), wq_old.dtype),
            jax.ShapeDtypeStruct((rows, columns), jnp.float32),
            jax.ShapeDtypeStruct(wkv.shape, wkv.dtype),
            jax.ShapeDtypeStruct((rows, width), jnp.float32),
        ),
        grid_spec=pltpu.PrefetchScalarGridSpec(
            num_scalar_prefetch=1,
            grid=(sections * steps,),
            in_specs=[
                pl.BlockSpec((rows, total_depth), lambda i, me: (0, 0)),
                pl.BlockSpec((rows, columns), lambda i, me: (0, 0)),
                pl.BlockSpec((tile, columns), own_at),
                pl.BlockSpec((tile, columns), far_at),
                pl.BlockSpec(early.shape, lambda i, me: (0, 0)),
                pl.BlockSpec((tile, width), lambda i, me: (i, 0)),
            ],
            out_specs=(
                pl.BlockSpec((tile, columns), lambda i, me: (i, 0)),
                pl.BlockSpec((rows, columns), lambda i, me: (0, 0)),
                pl.BlockSpec((tile, width), lambda i, me: (i, 0)),
                pl.BlockSpec((rows, width), lambda i, me: (0, 0)),
            ),
            scratch_shapes=[
                pltpu.VMEM((rows, columns), jnp.float32),
                pltpu.VMEM((rows, width), jnp.float32),
            ],
        ),
        cost_estimate=pl.CostEstimate(
            flops=2 * rows * total_depth * columns,
            bytes_accessed=4 * total_depth * columns,
            transcendentals=0,
        ),
        compiler_params=pltpu.CompilerParams(vmem_limit_bytes=VMEM_LIMIT),
        name="gather_query",
    )(me, normed, part, wq_old, far, early, wkv)


def place_kernel(sections, depth, late_ref, held_ref, out_ref, done):
    me = lax.axis_index("section")
    pieces = done.shape[0]
    piece = late_ref.shape[0] // pieces
    feeder = jnp.where(me == 0, 1, sections - 2)
    start = feeder * depth + depth - late_ref.shape[0]

    def write(p):
        return pltpu.make_async_copy(
            late_ref.at[pl.ds(p * piece, piece), :],
            out_ref.at[pl.ds(pl.multiple_of(start + p * piece, 16), piece), :],
            done.at[p],
        )

    @pl.when(jnp.logical_or(me == 0, me == sections - 1))
    def _():
        for p in range(pieces):
            write(p).start()
        for p in range(pieces):
            write(p).wait()


def place_late(late, wq_new, sections):
    depth = wq_new.shape[0] // sections
    hbm = pl.BlockSpec(memory_space=pl.ANY)
    return pl.pallas_call(
        functools.partial(place_kernel, sections, depth),
        out_shape=jax.ShapeDtypeStruct(wq_new.shape, wq_new.dtype),
        in_specs=[pl.BlockSpec(memory_space=pltpu.VMEM), hbm],
        out_specs=hbm,
        scratch_shapes=[pltpu.SemaphoreType.DMA((2,))],
        input_output_aliases={1: 0},
        cost_estimate=pl.CostEstimate(
            flops=1024, bytes_accessed=4 * late.size, transcendentals=0
        ),
        compiler_params=pltpu.CompilerParams(vmem_limit_bytes=16 * 2**20),
        name="place_late",
    )(late, wq_new)


def take_kernel(start, from_ref, out_ref, done):
    copy = pltpu.make_async_copy(from_ref.at[pl.ds(start, out_ref.shape[0]), :], out_ref, done)
    copy.start()
    copy.wait()


def take_rows(array, start, rows):
    return pl.pallas_call(
        functools.partial(take_kernel, start),
        out_shape=jax.ShapeDtypeStruct((rows, array.shape[1]), array.dtype),
        in_specs=[pl.BlockSpec(memory_space=pl.ANY)],
        out_specs=pl.BlockSpec(memory_space=pltpu.VMEM),
        scratch_shapes=[pltpu.SemaphoreType.DMA],
        compiler_params=pltpu.CompilerParams(vmem_limit_bytes=VMEM_LIMIT),
        name="take_rows",
    )(array)


def attend_kernel(
    pages_of, together, page, head_dim, block_ref, spot_ref, length_ref, in_ref, fresh_ref, query_ref, cache_ref, context_ref, mixed
):
    step = pl.program_id(0)

    def order(j, carry):
        start = pl.multiple_of(j * page, page)
        for r in range(together):
            at = (step * together + r) * pages_of + j
            cache_ref[r, pl.ds(start, page), :] = in_ref[block_ref[at], r, spot_ref[at]]
        return carry

    lax.fori_loop(0, pages_of, order, 0, unroll=8)
    for r in range(together):
        length = length_ref[step * together + r]
        start = pl.multiple_of(lax.div(length, page) * page, page)
        held = cache_ref[r, pl.ds(start, page), :]
        row = lax.broadcasted_iota(jnp.int32, held.shape, 0)
        fresh = jnp.broadcast_to(fresh_ref[r].astype(jnp.float32), held.shape)
        cache_ref[r, pl.ds(start, page), :] = jnp.where(
            row == lax.rem(length, page), fresh, held.astype(jnp.float32)
        ).astype(held.dtype)
    scores = [
        lax.dot_general(
            query_ref[r],
            cache_ref[r, :, :head_dim],
            (((1,), (1,)), ((), ())),
            preferred_element_type=jnp.float32,
        )
        * head_dim ** (-0.5)
        for r in range(together)
    ]
    seen = [
        lax.broadcasted_iota(jnp.int32, scores[r].shape, 1) <= length_ref[step * together + r]
        for r in range(together)
    ]
    peak = [
        jnp.max(jnp.where(seen[r], scores[r], -jnp.inf), axis=1, keepdims=True)
        for r in range(together)
    ]
    weights = [jnp.where(seen[r], jnp.exp(scores[r] - peak[r]), 0.0) for r in range(together)]
    sums = [jnp.sum(weights[r], axis=1, keepdims=True) for r in range(together)]
    probs = [(weights[r] / sums[r]).astype(jnp.bfloat16) for r in range(together)]
    for r in range(together):
        mixed[step * together + r] = jnp.dot(
            probs[r], cache_ref[r, :, head_dim:], preferred_element_type=jnp.float32
        )

    @pl.when(step == pl.num_programs(0) - 1)
    def _():
        for head in range(mixed.shape[1]):
            context_ref[:, pl.ds(head * head_dim, head_dim)] = mixed[:, head].astype(
                context_ref.dtype
            )


def attend(arrived, block, spot, lengths, fresh, query, head_dim):
    blocks, rows, per_block, page, width = arrived.shape
    pages_of = blocks * per_block
    heads = query.shape[1]
    together = next(n for n in (TOGETHER, 2, 1) if rows % n == 0)
    return pl.pallas_call(
        functools.partial(attend_kernel, pages_of, together, page, head_dim),
        out_shape=(
            jax.ShapeDtypeStruct((rows, pages_of * page, width), arrived.dtype),
            jax.ShapeDtypeStruct((rows, heads * head_dim), jnp.bfloat16),
        ),
        grid_spec=pltpu.PrefetchScalarGridSpec(
            num_scalar_prefetch=3,
            grid=(rows // together,),
            in_specs=[
                pl.BlockSpec(
                    (blocks, together, per_block, page, width), lambda r, *_: (0, r, 0, 0, 0)
                ),
                pl.BlockSpec((together, 1, width), lambda r, *_: (r, 0, 0)),
                pl.BlockSpec((together, heads, head_dim), lambda r, *_: (r, 0, 0)),
            ],
            out_specs=(
                pl.BlockSpec((together, pages_of * page, width), lambda r, *_: (r, 0, 0)),
                pl.BlockSpec((rows, heads * head_dim), lambda r, *_: (0, 0)),
            ),
            scratch_shapes=[pltpu.VMEM((rows, heads, head_dim), jnp.float32)],
        ),
        cost_estimate=pl.CostEstimate(
            flops=4 * rows * heads * pages_of * page * head_dim,
            bytes_accessed=4 * arrived.size,
            transcendentals=rows * heads * pages_of * page,
        ),
        compiler_params=pltpu.CompilerParams(vmem_limit_bytes=VMEM_LIMIT),
        name="attend",
    )(block.reshape(-1), spot.reshape(-1), lengths, arrived, fresh[:, None, :], query)


def work(hidden_state, norm_gain, wq_old, wkv_old, kv_old, page_table, lengths):
    sections = lax.axis_size("section")
    tensors = lax.axis_size("tensor")
    section_id = lax.axis_index("section")
    tensor_id = lax.axis_index("tensor")
    rows = hidden_state.shape[0]
    head_dim = HEAD_DIM
    width = 2 * head_dim
    repeats = tensors // KV_HEADS
    queries_here = wq_old.shape[1] // head_dim
    pool_dev = kv_old.shape[1]
    page = kv_old.shape[2]
    per_block = page_table.shape[1] // tensors
    widened = hidden_state.astype(jnp.float32)
    scale = lax.rsqrt(jnp.mean(widened * widened, axis=1, keepdims=True) + EPSILON)
    normed = (widened * scale * norm_gain[None, :]).astype(jnp.bfloat16)
    owner = page_table // pool_dev
    blocks = jnp.arange(tensors, dtype=jnp.int32)
    onehot = (owner[:, :, None] == blocks[None, None, :]).astype(jnp.int32)
    ranks = jnp.sum((jnp.cumsum(onehot, axis=1) - 1) * onehot, axis=2)
    mine = owner == tensor_id
    wanted = ranks[:, :, None] == jnp.arange(per_block, dtype=jnp.int32)[None, None, :]
    picks = (mine[:, :, None] & wanted).astype(jnp.int32)
    spots = jnp.sum(picks * (page_table % pool_dev)[:, :, None], axis=1)
    pages = pick_pages(kv_old, spots.reshape(-1), sections)
    depth = wq_old.shape[0]
    ends = sorted({(sections - 2, sections - 1), (1, 0)})
    tiles, early_tiles, late_tiles = split(depth)
    early = take_rows(
        wq_old, (tiles - early_tiles - late_tiles) * UNIT, early_tiles * UNIT
    )
    early = lax.ppermute(early, "section", ends)
    part, arrived, wkv_far, far, _, _, late = exchange(
        normed, wq_old, pages, wkv_old, sections, tensors, repeats
    )
    late = lax.ppermute(late, "section", ends)
    me = jnp.full((1,), section_id, jnp.int32)
    wq_new, query, wkv_new, fresh = gather(
        me, normed, part, wq_old, far, early, wkv_far, sections
    )
    arrived = arrived.reshape(tensors, rows, per_block, page, width)
    block = lax.dynamic_slice_in_dim(owner, section_id * rows, rows, 0)
    spot = lax.dynamic_slice_in_dim(ranks, section_id * rows, rows, 0)
    my_lengths = lax.dynamic_slice_in_dim(lengths, section_id * rows, rows, 0)
    fresh_key = rotate(fresh[:, None, :head_dim], my_lengths, head_dim)[:, 0]
    fresh = jnp.concatenate([fresh_key, fresh[:, head_dim:]], axis=1).astype(jnp.bfloat16)
    query = rotate(query.reshape(rows, queries_here, head_dim), my_lengths, head_dim).astype(
        jnp.bfloat16
    )
    cache, context = attend(arrived, block, spot, my_lengths, fresh, query, head_dim)
    wq_new = place_late(late, wq_new, sections)
    return (context, cache[:, None], wq_new, wkv_new)


def solution(mesh):
    placed = (
        P("section", None),
        P(),
        P("section", "tensor"),
        P("tensor", "section"),
        P("section", "tensor", None, None),
        P(),
        P(),
    )
    return jax.shard_map(
        work,
        mesh=mesh,
        in_specs=placed,
        out_specs=(
            P("section", "tensor"),
            P("section", "tensor", None, None),
            P(None, "tensor"),
            P(None, "tensor"),
        ),
        check_vma=False,
    )
```

```python
import functools

import jax
import jax.numpy as jnp
from jax import lax
from jax.experimental import pallas as pl
from jax.experimental.pallas import tpu as pltpu
from jax.sharding import PartitionSpec as P


KV_HEADS = 8
HEAD_DIM = 128


EPSILON = 1e-05
ROPE_BASE = 500000.0
MESH = pl.DeviceIdType.MESH
CHUNKS = 16
PIECES = 4
STAGGER = 3
UNIT = 128
EARLY = 4
LATE = 7
PAIR = 8
TOGETHER = 4
VMEM_LIMIT = 60 * 2**20


def split(depth):
    tiles = depth // UNIT
    return tiles, max(1, tiles * EARLY // 16), max(1, tiles * LATE // 16)


def rotate(values, position, head_dim):
    half = head_dim // 2
    frequency = ROPE_BASE ** (-(jnp.arange(half, dtype=jnp.float32) * 2.0 / head_dim))
    angles = position.astype(jnp.float32)[:, None] * frequency[None, :]
    cosine = jnp.cos(angles)[:, None, :]
    sine = jnp.sin(angles)[:, None, :]
    first = values[..., :half]
    second = values[..., half:]
    return jnp.concatenate(
        [first * cosine - second * sine, second * cosine + first * sine], axis=-1
    )


def pick_kernel(count, spots_ref, kv_ref, out_ref):
    base = pl.program_id(1) * count

    def step(i, carry):
        out_ref[0, 0, i] = kv_ref[0, spots_ref[base + i]]
        return carry

    lax.fori_loop(0, count, step, 0, unroll=32)


def pick_pages(kv_old, spots, sections):
    heads, pool, page, width = kv_old.shape
    count = spots.shape[0] // sections
    return pl.pallas_call(
        functools.partial(pick_kernel, count),
        out_shape=jax.ShapeDtypeStruct((sections, heads, count, page, width), kv_old.dtype),
        grid_spec=pltpu.PrefetchScalarGridSpec(
            num_scalar_prefetch=1,
            grid=(heads, sections),
            in_specs=[pl.BlockSpec((1, pool, page, width), lambda h, s, spots: (h, 0, 0, 0))],
            out_specs=pl.BlockSpec(
                (1, 1, count, page, width), lambda h, s, spots: (s, h, 0, 0, 0)
            ),
        ),
        compiler_params=pltpu.CompilerParams(vmem_limit_bytes=VMEM_LIMIT),
        name="pick_pages",
    )(spots, kv_old)


def exchange_kernel(
    sections,
    tensors,
    local_heads,
    repeats,
    kept,
    normed_ref,
    wq_ref,
    pages_ref,
    wkv_ref,
    part_ref,
    arrived_ref,
    wkv_new_ref,
    wq_new_ref,
    stage_ref,
    stage_wkv_ref,
    late_ref,
    held,
    spread,
    made,
    part_in,
    page_send,
    page_recv,
    wkv_send,
    wkv_recv,
    local_sem,
    own_send,
    relay_send,
    wq_recv,
    stage_send,
    stage_recv,
    wkv_own_send,
    wkv_relay_send,
    wkv_stage_recv,
    help_send,
    help_recv,
    turn,
):
    me = lax.axis_index("section")
    mine = lax.axis_index("tensor")
    depth, columns = wq_ref.shape
    width = wkv_new_ref.shape[1]
    block = wkv_ref.shape[0]
    late_rows = late_ref.shape[0]
    chunks = own_send.shape[1]
    chunk = depth // chunks
    last = sections - 1
    onward = (me < last, me > 0)
    next_to = (me + 1, me - 1)
    feeds = (me == last - 1, me == 1)
    fed = (me == last, me == 0)

    def wq_rows(owner, i):
        return wq_new_ref.at[pl.ds(pl.multiple_of(owner * depth + i * chunk, 16), chunk), :]

    def own_copy(side, i):
        return pltpu.make_async_remote_copy(
            wq_ref.at[pl.ds(pl.multiple_of(i * chunk, 16), chunk), :],
            wq_rows(me, i),
            own_send.at[side, i],
            wq_recv.at[me, i],
            device_id=(next_to[side], mine),
            device_id_type=MESH,
        )

    def relay_copy(owner, side, i):
        return pltpu.make_async_remote_copy(
            wq_rows(owner, i),
            wq_rows(owner, i),
            relay_send.at[owner, i],
            wq_recv.at[owner, i],
            device_id=(next_to[side], mine),
            device_id_type=MESH,
        )

    def each_chunk(act, first=0, end=chunks):
        def run(i, carry):
            act(i)
            return carry

        lax.fori_loop(first, end, run, 0)

    def goes(side, i):
        return jnp.logical_and(
            onward[side], jnp.logical_or(jnp.logical_not(feeds[side]), i < kept)
        )

    def send_own(i):
        for side in range(2):
            pl.when(goes(side, i))(lambda: own_copy(side, i).start())

    def owner_of(side, step):
        return (me - step, me + step)[side]

    def real(side, step):
        return (me - step >= 0, me + step < sections)[side]

    def stage_copy(origin, other, step):
        return pltpu.make_async_remote_copy(
            pages_ref.at[other],
            stage_ref.at[origin],
            stage_send.at[step],
            stage_recv.at[origin],
            device_id=(other, mine),
            device_id_type=MESH,
        )

    part_rows = block // PIECES

    def wkv_own_copy(side, p):
        return pltpu.make_async_remote_copy(
            wkv_ref.at[pl.ds(p * part_rows, part_rows), :],
            stage_wkv_ref.at[me, pl.ds(p * part_rows, part_rows), :],
            wkv_own_send.at[side, p],
            wkv_stage_recv.at[me, p],
            device_id=(next_to[side], mine),
            device_id_type=MESH,
        )

    def wkv_relay_copy(owner, side, p):
        here = stage_wkv_ref.at[owner, pl.ds(p * part_rows, part_rows), :]
        return pltpu.make_async_remote_copy(
            here,
            here,
            wkv_relay_send.at[owner, p],
            wkv_stage_recv.at[owner, p],
            device_id=(next_to[side], mine),
            device_id_type=MESH,
        )

    def page_copy(step, head, copy):
        slot = (step * local_heads + head) * repeats + copy
        other = lax.rem(me + step, sections)
        target = (other * local_heads + head) * repeats + copy
        source = pages_ref.at[me, head] if step == 0 else stage_ref.at[other, head]
        here = (source, arrived_ref.at[mine])
        remote = pltpu.make_async_remote_copy(
            *here,
            page_send.at[slot],
            page_recv.at[mine],
            device_id=(me, target),
            device_id_type=MESH,
        )
        return target, remote, pltpu.make_async_copy(*here, local_sem.at[0])

    def wkv_copy(step, head, copy):
        slot = (step * local_heads + head) * repeats + copy
        other = lax.rem(me + step, sections)
        target = (other * local_heads + head) * repeats + copy
        here = (
            (wkv_ref if step == 0 else stage_wkv_ref.at[other]).at[:, pl.ds(head * width, width)],
            wkv_new_ref.at[pl.ds(pl.multiple_of(mine * block, 128), block), :],
        )
        remote = pltpu.make_async_remote_copy(
            *here,
            wkv_send.at[slot],
            wkv_recv.at[mine],
            device_id=(me, target),
            device_id_type=MESH,
        )
        return target, remote, pltpu.make_async_copy(*here, local_sem.at[1])

    def begin(make, step):
        for head in range(local_heads):
            for copy in range(repeats):
                target, remote, local = make(step, head, copy)
                pl.when(target != mine)(remote.start)
                pl.when(target == mine)(local.start)

    def spread_copy(side):
        feeder = (last - 1, 1)[side]
        start = pl.multiple_of(feeder * depth + depth - late_rows, 128)
        return pltpu.make_async_remote_copy(
            normed_ref.at[:, pl.ds(start, late_rows)],
            spread.at[side],
            help_send.at[0],
            help_recv.at[side],
            device_id=(feeder, mine),
            device_id_type=MESH,
        )

    def part_copy(side):
        return pltpu.make_async_remote_copy(
            made.at[side],
            part_in,
            help_send.at[1 + side],
            help_recv.at[2],
            device_id=((last, 0)[side], mine),
            device_id_type=MESH,
        )

    for side in range(2):
        pl.when(fed[side])(lambda: spread_copy(side).start())
    begin(wkv_copy, 0)
    begin(page_copy, 0)
    second = lax.rem(mine, 2) == 1
    pl.when(second)(lambda: pl.semaphore_wait(turn, 1))
    for side in range(2):
        for p in range(PIECES):
            pl.when(onward[side])(lambda: wkv_own_copy(side, p).start())
    ahead = CHUNKS * 6 // 8
    each_chunk(send_own, 0, ahead)
    for step in range(sections - 1, 0, -1):
        for side in range(2):
            pl.when(real(side, step))(
                lambda: stage_copy(
                    me, owner_of(side, step), step if side else sections - step
                ).start()
            )
    each_chunk(send_own, ahead)

    @pl.when(jnp.logical_not(second))
    def _():
        for side in range(2):
            for p in range(STAGGER):
                pl.when(onward[side])(lambda: wkv_own_copy(side, p).wait_send())
        pl.semaphore_signal(turn, 1, device_id=(me, mine + 1), device_id_type=MESH)

    take = pltpu.make_async_copy(
        wq_ref.at[pl.ds(depth - late_rows, late_rows), :], held, local_sem.at[2]
    )
    take.start()
    take.wait()
    put = pltpu.make_async_copy(held, late_ref, local_sem.at[3])
    put.start()
    tile = 256
    for side in range(2):

        @pl.when(feeds[side])
        def _():
            spread_copy(side).wait_recv()

            def product(i, carry):
                span = pl.ds(pl.multiple_of(i * tile, tile), tile)
                made[side, :, span] = jnp.dot(
                    spread[side], held[:, span], preferred_element_type=jnp.float32
                )
                return carry

            lax.fori_loop(0, columns // tile, product, 0)
            part_copy(side).start()

    def pass_wkv(step):
        for p in range(PIECES):
            for side in range(2):
                owner = owner_of(side, step)

                @pl.when(real(side, step))
                def _():
                    wkv_relay_copy(owner, side, p).wait_recv()
                    pl.when(onward[side])(lambda: wkv_relay_copy(owner, side, p).start())

        for side in range(2):
            pl.when(real(side, step))(
                lambda: begin(wkv_copy, step if side else sections - step)
            )

    def pass_wq(step, first=0, stop=chunks):
        def pass_on(i):
            for side in range(2):
                owner = owner_of(side, step)
                there = real(side, step)
                if step == 1:
                    there = jnp.logical_and(
                        there, jnp.logical_or(jnp.logical_not(fed[side]), i < kept)
                    )

                @pl.when(there)
                def _():
                    relay_copy(owner, side, i).wait_recv()
                    pl.when(onward[side])(lambda: relay_copy(owner, side, i).start())

        each_chunk(pass_on, first, stop)

    def spread_pages(away, other):
        stage_copy(other, other, away).wait_recv()
        begin(page_copy, away)

    pass_wkv(1)
    pass_wq(1, 0, ahead)
    for step in range(sections - 1, 0, -1):
        for side in range(2):
            pl.when(real(side, step))(
                lambda: spread_pages(
                    step if side else sections - step, owner_of(side, step)
                )
            )
    pass_wq(1, ahead)
    for step in range(2, sections):
        pass_wkv(step)
        if step < last:
            pass_wq(step)

    put.wait()
    for side in range(2):

        @pl.when(fed[side])
        def _():
            spread_copy(side).wait_send()
            part_copy(side).wait_recv()

        pl.when(feeds[side])(lambda: part_copy(side).wait_send())
    end = jnp.logical_or(fed[0], fed[1])

    @pl.when(end)
    def _():
        part_ref[...] = part_in[...]

    @pl.when(jnp.logical_not(end))
    def _():
        part_ref[...] = jnp.zeros_like(part_ref)

    def sent(i):
        for side in range(2):
            pl.when(goes(side, i))(lambda: own_copy(side, i).wait_send())
            for step in range(1, sections):
                pl.when(jnp.logical_and(real(side, step), onward[side]))(
                    lambda: relay_copy(owner_of(side, step), side, i).wait_send()
                )

    each_chunk(sent)
    for side in range(2):
        for p in range(PIECES):
            pl.when(jnp.logical_and(onward[side], jnp.logical_or(second, p >= STAGGER)))(
                lambda: wkv_own_copy(side, p).wait_send()
            )
            for step in range(1, sections):
                pl.when(jnp.logical_and(real(side, step), onward[side]))(
                    lambda: wkv_relay_copy(owner_of(side, step), side, p).wait_send()
                )
    for step in range(1, sections):
        stage_copy(me, lax.rem(me + step, sections), step).wait_send()
    for make in (page_copy, wkv_copy):
        for step in range(sections):
            for head in range(local_heads):
                for copy in range(repeats):
                    target, remote, local = make(step, head, copy)
                    pl.when(target != mine)(remote.wait_send)
                    pl.when(target == mine)(local.wait)
    for origin in range(tensors):
        pages_in = pltpu.make_async_remote_copy(
            pages_ref.at[0, 0],
            arrived_ref.at[origin],
            page_send.at[0],
            page_recv.at[origin],
            device_id=(me, origin),
            device_id_type=MESH,
        )
        wkv_in = pltpu.make_async_remote_copy(
            wkv_ref.at[:, pl.ds(0, width)],
            wkv_new_ref.at[pl.ds(origin * block, block), :],
            wkv_send.at[0],
            wkv_recv.at[origin],
            device_id=(me, origin),
            device_id_type=MESH,
        )
        outside = mine != origin
        pl.when(outside)(pages_in.wait_recv)
        pl.when(outside)(wkv_in.wait_recv)
    if last > 1:
        pass_wq(last)


def exchange(normed, wq_old, pages, wkv_old, sections, tensors, repeats):
    rows = normed.shape[0]
    depth, columns = wq_old.shape
    local_heads = pages.shape[1]
    width = pages.shape[4]
    copies = sections * local_heads * repeats
    tiles, early, late = split(depth)
    late_rows = late * UNIT
    kept = (tiles - early - late) * UNIT * CHUNKS // depth
    dma = pltpu.SemaphoreType.DMA
    vmem = pl.BlockSpec(memory_space=pltpu.VMEM)
    hbm = pl.BlockSpec(memory_space=pl.ANY)
    return pl.pallas_call(
        functools.partial(
            exchange_kernel, sections, tensors, local_heads, repeats, kept
        ),
        out_shape=(
            jax.ShapeDtypeStruct((rows, columns), jnp.float32),
            jax.ShapeDtypeStruct((tensors,) + pages.shape[2:], pages.dtype),
            jax.ShapeDtypeStruct((wkv_old.shape[0] * tensors, width), wkv_old.dtype),
            jax.ShapeDtypeStruct((depth * sections, columns), wq_old.dtype),
            jax.ShapeDtypeStruct(pages.shape, pages.dtype),
            jax.ShapeDtypeStruct((sections,) + wkv_old.shape, wkv_old.dtype),
            jax.ShapeDtypeStruct((late_rows, columns), wq_old.dtype),
        ),
        in_specs=[vmem, hbm, hbm, hbm],
        out_specs=(vmem, hbm, hbm, hbm, hbm, hbm, hbm),
        scratch_shapes=[
            pltpu.VMEM((late_rows, columns), wq_old.dtype),
            pltpu.VMEM((2, rows, late_rows), normed.dtype),
            pltpu.VMEM((2, rows, columns), jnp.float32),
            pltpu.VMEM((rows, columns), jnp.float32),
            dma((copies,)),
            dma((tensors,)),
            dma((copies,)),
            dma((tensors,)),
            dma((4,)),
            dma((2, CHUNKS)),
            dma((sections, CHUNKS)),
            dma((sections, CHUNKS)),
            dma((sections,)),
            dma((sections,)),
            dma((2, PIECES)),
            dma((sections, PIECES)),
            dma((sections, PIECES)),
            dma((3,)),
            dma((3,)),
            pltpu.SemaphoreType.REGULAR,
        ],
        compiler_params=pltpu.CompilerParams(
            has_side_effects=True, vmem_limit_bytes=VMEM_LIMIT
        ),
        cost_estimate=pl.CostEstimate(
            flops=4 * rows * late_rows * columns,
            bytes_accessed=400 * 2**20,
            transcendentals=0,
        ),
        name="exchange",
    )(normed, wq_old, pages, wkv_old)


def gather_kernel(
    sections,
    tiles,
    first,
    last,
    pair,
    me_ref,
    normed_ref,
    part_ref,
    own_ref,
    far_ref,
    early_ref,
    wkv_ref,
    out_ref,
    query_ref,
    wkv_out_ref,
    fresh_ref,
    total,
    fresh,
):
    i = pl.program_id(0)
    me = me_ref[0]
    owner = i // (tiles // pair)
    tile = UNIT
    mine = owner == me
    fed = jnp.logical_or(
        jnp.logical_and(me == sections - 1, owner == sections - 2),
        jnp.logical_and(me == 0, owner == 1),
    )

    @pl.when(i == 0)
    def _():
        total[...] = part_ref[...]
        fresh[...] = jnp.zeros_like(fresh)

    def keep(ref, rows, at):
        out_ref[pl.ds(at * tile, tile), :] = ref[rows, :]

    for at in range(pair):
        k = (i % (tiles // pair)) * pair + at
        rows = pl.ds(at * tile, tile)
        early = jnp.logical_and(fed, jnp.logical_and(k >= first, k < last))
        late = jnp.logical_and(fed, k >= last)
        start = jnp.clip(k - first, 0, last - first - 1) * tile
        other = jnp.logical_or(mine, jnp.logical_or(early, late))
        pl.when(mine)(lambda: keep(own_ref, rows, at))
        pl.when(early)(
            lambda: keep(early_ref, pl.ds(pl.multiple_of(start, UNIT), tile), at)
        )
        pl.when(jnp.logical_not(other))(lambda: keep(far_ref, rows, at))

        @pl.when(late)
        def _():
            out_ref[rows, :] = jnp.zeros((tile, out_ref.shape[1]), out_ref.dtype)

    span = pl.ds(pl.multiple_of(i * pair * tile, UNIT), pair * tile)
    features = normed_ref[:, span]
    total[...] += jnp.dot(features, out_ref[...], preferred_element_type=jnp.float32)
    wkv_out_ref[...] = wkv_ref[...]
    fresh[...] += jnp.dot(features, wkv_ref[...], preferred_element_type=jnp.float32)

    @pl.when(i == pl.num_programs(0) - 1)
    def _():
        query_ref[...] = total[...]
        fresh_ref[...] = fresh[...]


def gather(me, normed, part, wq_old, far, early, wkv, sections):
    rows, total_depth = normed.shape
    depth, columns = wq_old.shape
    tiles, early_tiles, late_tiles = split(depth)
    pair = min(PAIR, tiles)
    steps = tiles // pair
    tile = pair * UNIT
    width = wkv.shape[1]

    def own_at(i, me):
        return (jnp.clip(i - me[0] * steps, 0, steps - 1), 0)

    def far_at(i, me):
        own = i // steps == me[0]
        return (jnp.where(own, jnp.maximum(me[0] * steps - 1, 0), i), 0)

    return pl.pallas_call(
        functools.partial(
            gather_kernel,
            sections,
            tiles,
            tiles - early_tiles - late_tiles,
            tiles - late_tiles,
            pair,
        ),
        out_shape=(
            jax.ShapeDtypeStruct((total_depth, columns), wq_old.dtype),
            jax.ShapeDtypeStruct((rows, columns), jnp.float32),
            jax.ShapeDtypeStruct(wkv.shape, wkv.dtype),
            jax.ShapeDtypeStruct((rows, width), jnp.float32),
        ),
        grid_spec=pltpu.PrefetchScalarGridSpec(
            num_scalar_prefetch=1,
            grid=(sections * steps,),
            in_specs=[
                pl.BlockSpec((rows, total_depth), lambda i, me: (0, 0)),
                pl.BlockSpec((rows, columns), lambda i, me: (0, 0)),
                pl.BlockSpec((tile, columns), own_at),
                pl.BlockSpec((tile, columns), far_at),
                pl.BlockSpec(early.shape, lambda i, me: (0, 0)),
                pl.BlockSpec((tile, width), lambda i, me: (i, 0)),
            ],
            out_specs=(
                pl.BlockSpec((tile, columns), lambda i, me: (i, 0)),
                pl.BlockSpec((rows, columns), lambda i, me: (0, 0)),
                pl.BlockSpec((tile, width), lambda i, me: (i, 0)),
                pl.BlockSpec((rows, width), lambda i, me: (0, 0)),
            ),
            scratch_shapes=[
                pltpu.VMEM((rows, columns), jnp.float32),
                pltpu.VMEM((rows, width), jnp.float32),
            ],
        ),
        cost_estimate=pl.CostEstimate(
            flops=2 * rows * total_depth * columns,
            bytes_accessed=4 * total_depth * columns,
            transcendentals=0,
        ),
        compiler_params=pltpu.CompilerParams(vmem_limit_bytes=VMEM_LIMIT),
        name="gather_query",
    )(me, normed, part, wq_old, far, early, wkv)


def place_kernel(sections, depth, late_ref, held_ref, out_ref, done):
    me = lax.axis_index("section")
    pieces = done.shape[0]
    piece = late_ref.shape[0] // pieces
    feeder = jnp.where(me == 0, 1, sections - 2)
    start = feeder * depth + depth - late_ref.shape[0]

    def write(p):
        return pltpu.make_async_copy(
            late_ref.at[pl.ds(p * piece, piece), :],
            out_ref.at[pl.ds(pl.multiple_of(start + p * piece, 16), piece), :],
            done.at[p],
        )

    @pl.when(jnp.logical_or(me == 0, me == sections - 1))
    def _():
        for p in range(pieces):
            write(p).start()
        for p in range(pieces):
            write(p).wait()


def place_late(late, wq_new, sections):
    depth = wq_new.shape[0] // sections
    hbm = pl.BlockSpec(memory_space=pl.ANY)
    return pl.pallas_call(
        functools.partial(place_kernel, sections, depth),
        out_shape=jax.ShapeDtypeStruct(wq_new.shape, wq_new.dtype),
        in_specs=[pl.BlockSpec(memory_space=pltpu.VMEM), hbm],
        out_specs=hbm,
        scratch_shapes=[pltpu.SemaphoreType.DMA((2,))],
        input_output_aliases={1: 0},
        cost_estimate=pl.CostEstimate(
            flops=1024, bytes_accessed=4 * late.size, transcendentals=0
        ),
        compiler_params=pltpu.CompilerParams(vmem_limit_bytes=16 * 2**20),
        name="place_late",
    )(late, wq_new)


def take_kernel(sections, start, from_ref, out_ref, done):
    me = lax.axis_index("section")

    @pl.when(jnp.logical_or(me == 1, me == sections - 2))
    def _():
        copy = pltpu.make_async_copy(
            from_ref.at[pl.ds(start, out_ref.shape[0]), :], out_ref, done
        )
        copy.start()
        copy.wait()


def take_rows(array, start, rows, sections):
    return pl.pallas_call(
        functools.partial(take_kernel, sections, start),
        out_shape=jax.ShapeDtypeStruct((rows, array.shape[1]), array.dtype),
        in_specs=[pl.BlockSpec(memory_space=pl.ANY)],
        out_specs=pl.BlockSpec(memory_space=pltpu.VMEM),
        scratch_shapes=[pltpu.SemaphoreType.DMA],
        compiler_params=pltpu.CompilerParams(vmem_limit_bytes=VMEM_LIMIT),
        name="take_rows",
    )(array)


def attend_kernel(
    pages_of, together, page, head_dim, block_ref, spot_ref, length_ref, in_ref, fresh_ref, query_ref, cache_ref, context_ref, mixed
):
    step = pl.program_id(0)

    def order(j, carry):
        start = pl.multiple_of(j * page, page)
        for r in range(together):
            at = (step * together + r) * pages_of + j
            cache_ref[r, pl.ds(start, page), :] = in_ref[block_ref[at], r, spot_ref[at]]
        return carry

    lax.fori_loop(0, pages_of, order, 0, unroll=16)
    for r in range(together):
        length = length_ref[step * together + r]
        start = pl.multiple_of(lax.div(length, page) * page, page)
        held = cache_ref[r, pl.ds(start, page), :]
        row = lax.broadcasted_iota(jnp.int32, held.shape, 0)
        fresh = jnp.broadcast_to(fresh_ref[r].astype(jnp.float32), held.shape)
        cache_ref[r, pl.ds(start, page), :] = jnp.where(
            row == lax.rem(length, page), fresh, held.astype(jnp.float32)
        ).astype(held.dtype)
    scores = [
        lax.dot_general(
            query_ref[r],
            cache_ref[r, :, :head_dim],
            (((1,), (1,)), ((), ())),
            preferred_element_type=jnp.float32,
        )
        * head_dim ** (-0.5)
        for r in range(together)
    ]
    seen = [
        lax.broadcasted_iota(jnp.int32, scores[r].shape, 1) <= length_ref[step * together + r]
        for r in range(together)
    ]
    peak = [
        jnp.max(jnp.where(seen[r], scores[r], -jnp.inf), axis=1, keepdims=True)
        for r in range(together)
    ]
    weights = [jnp.where(seen[r], jnp.exp(scores[r] - peak[r]), 0.0) for r in range(together)]
    sums = [jnp.sum(weights[r], axis=1, keepdims=True) for r in range(together)]
    probs = [(weights[r] / sums[r]).astype(jnp.bfloat16) for r in range(together)]
    for r in range(together):
        mixed[step * together + r] = jnp.dot(
            probs[r], cache_ref[r, :, head_dim:], preferred_element_type=jnp.float32
        )

    @pl.when(step == pl.num_programs(0) - 1)
    def _():
        for head in range(mixed.shape[1]):
            context_ref[:, pl.ds(head * head_dim, head_dim)] = mixed[:, head].astype(
                context_ref.dtype
            )


def attend(arrived, block, spot, lengths, fresh, query, head_dim):
    blocks, rows, per_block, page, width = arrived.shape
    pages_of = blocks * per_block
    heads = query.shape[1]
    together = next(n for n in (TOGETHER, 2, 1) if rows % n == 0)
    return pl.pallas_call(
        functools.partial(attend_kernel, pages_of, together, page, head_dim),
        out_shape=(
            jax.ShapeDtypeStruct((rows, pages_of * page, width), arrived.dtype),
            jax.ShapeDtypeStruct((rows, heads * head_dim), jnp.bfloat16),
        ),
        grid_spec=pltpu.PrefetchScalarGridSpec(
            num_scalar_prefetch=3,
            grid=(rows // together,),
            in_specs=[
                pl.BlockSpec(
                    (blocks, together, per_block, page, width), lambda r, *_: (0, r, 0, 0, 0)
                ),
                pl.BlockSpec((together, 1, width), lambda r, *_: (r, 0, 0)),
                pl.BlockSpec((together, heads, head_dim), lambda r, *_: (r, 0, 0)),
            ],
            out_specs=(
                pl.BlockSpec((together, pages_of * page, width), lambda r, *_: (r, 0, 0)),
                pl.BlockSpec((rows, heads * head_dim), lambda r, *_: (0, 0)),
            ),
            scratch_shapes=[pltpu.VMEM((rows, heads, head_dim), jnp.float32)],
        ),
        cost_estimate=pl.CostEstimate(
            flops=4 * rows * heads * pages_of * page * head_dim,
            bytes_accessed=4 * arrived.size,
            transcendentals=rows * heads * pages_of * page,
        ),
        compiler_params=pltpu.CompilerParams(vmem_limit_bytes=VMEM_LIMIT),
        name="attend",
    )(block.reshape(-1), spot.reshape(-1), lengths, arrived, fresh[:, None, :], query)


def work(hidden_state, norm_gain, wq_old, wkv_old, kv_old, page_table, lengths):
    sections = lax.axis_size("section")
    tensors = lax.axis_size("tensor")
    section_id = lax.axis_index("section")
    tensor_id = lax.axis_index("tensor")
    rows = hidden_state.shape[0]
    head_dim = HEAD_DIM
    width = 2 * head_dim
    repeats = tensors // KV_HEADS
    queries_here = wq_old.shape[1] // head_dim
    pool_dev = kv_old.shape[1]
    page = kv_old.shape[2]
    per_block = page_table.shape[1] // tensors
    widened = hidden_state.astype(jnp.float32)
    scale = lax.rsqrt(jnp.mean(widened * widened, axis=1, keepdims=True) + EPSILON)
    normed = (widened * scale * norm_gain[None, :]).astype(jnp.bfloat16)
    owner = page_table // pool_dev
    blocks = jnp.arange(tensors, dtype=jnp.int32)
    onehot = (owner[:, :, None] == blocks[None, None, :]).astype(jnp.int32)
    ranks = jnp.sum((jnp.cumsum(onehot, axis=1) - 1) * onehot, axis=2)
    mine = owner == tensor_id
    wanted = ranks[:, :, None] == jnp.arange(per_block, dtype=jnp.int32)[None, None, :]
    picks = (mine[:, :, None] & wanted).astype(jnp.int32)
    spots = jnp.sum(picks * (page_table % pool_dev)[:, :, None], axis=1)
    pages = pick_pages(kv_old, spots.reshape(-1), sections)
    depth = wq_old.shape[0]
    ends = sorted({(sections - 2, sections - 1), (1, 0)})
    tiles, early_tiles, late_tiles = split(depth)
    early = take_rows(
        wq_old, (tiles - early_tiles - late_tiles) * UNIT, early_tiles * UNIT, sections
    )
    early = lax.ppermute(early, "section", ends)
    part, arrived, wkv_far, far, _, _, late = exchange(
        normed, wq_old, pages, wkv_old, sections, tensors, repeats
    )
    late = lax.ppermute(late, "section", ends)
    me = jnp.full((1,), section_id, jnp.int32)
    wq_new, query, wkv_new, fresh = gather(
        me, normed, part, wq_old, far, early, wkv_far, sections
    )
    arrived = arrived.reshape(tensors, rows, per_block, page, width)
    block = lax.dynamic_slice_in_dim(owner, section_id * rows, rows, 0)
    spot = lax.dynamic_slice_in_dim(ranks, section_id * rows, rows, 0)
    my_lengths = lax.dynamic_slice_in_dim(lengths, section_id * rows, rows, 0)
    fresh_key = rotate(fresh[:, None, :head_dim], my_lengths, head_dim)[:, 0]
    fresh = jnp.concatenate([fresh_key, fresh[:, head_dim:]], axis=1).astype(jnp.bfloat16)
    query = rotate(query.reshape(rows, queries_here, head_dim), my_lengths, head_dim).astype(
        jnp.bfloat16
    )
    cache, context = attend(arrived, block, spot, my_lengths, fresh, query, head_dim)
    wq_new = place_late(late, wq_new, sections)
    return (context, cache[:, None], wq_new, wkv_new)


def solution(mesh):
    placed = (
        P("section", None),
        P(),
        P("section", "tensor"),
        P("tensor", "section"),
        P("section", "tensor", None, None),
        P(),
        P(),
    )
    return jax.shard_map(
        work,
        mesh=mesh,
        in_specs=placed,
        out_specs=(
            P("section", "tensor"),
            P("section", "tensor", None, None),
            P(None, "tensor"),
            P(None, "tensor"),
        ),
        check_vma=False,
    )
```
